32 devices in a mesh: rows: 16 (over z, x, core), chan: 2 (over y).
Axes of the slice: x: 2, y: 2, z: 4, core: 2. Of those that a mesh axis runs over, the one named last changes fastest.
Arguments:
- pixels: float32 [1024, 16384], P(('chan', 'rows')), parts along dimension 0, may hold values from -6 to 6
- row_taps: float32 [32768], P(('chan', 'rows')), parts along dimension 0, may hold values from -0.046875 to 0.046875
- column_taps: float32 [1024], P(('chan', 'rows')), parts along dimension 0, may hold values from -0.25 to 0.25
- stencil: float32 [6, 3], P('chan'), parts along dimension 0, may hold values from -3 to 3
Outputs:
- filtered: float32 [1024, 16384], P(('chan', 'rows')), parts along dimension 0
The draws below stay inside these ranges and needn't reach their ends.
There are 2 independent parts, one for each index of `chan`. The reference program is written for one: setup_inputs(seed, part) draws one part's arguments, and reference() takes and returns one part's arrays. A program takes and returns all parts, laid end to end along the dimension named above; each array names one. Nothing has to cross between parts.
All inputs are finite; a program needn't handle non-finite values.
Results may differ from the reference program's by a relative error of at most 0.0003.
Values sent between devices are 32-bit elements; how exact they have to be, the bound alone decides.
A program may use at most 128 MiB of HBM per device.

```python
import jax
import jax.numpy as jnp

NX = 16384
NY = 512


def steps_of(key, dims, shards, least, largest):
    def one(position, parts):
        heights = jax.random.uniform(jax.random.fold_in(jax.random.fold_in(key, 6), position), (parts,), jnp.float32, least / len(shards), largest / len(shards))
        return jnp.repeat(jnp.exp(heights), dims[position] // parts).reshape((-1,) + (1,) * (len(dims) - position - 1))

    loudness = one(*shards[0])
    for cut in shards[1:]:
        loudness = loudness * one(*cut)
    return loudness


def bell_draw(key, dims, scale, limit, pieces=(), kind=jnp.bfloat16):
    loudness = steps_of(key, dims, pieces, -0.22, 0.18) if pieces else 1.0
    values = jax.random.normal(key, dims, jnp.float32) * scale * loudness
    return jnp.minimum(jnp.maximum(values, -limit), limit).astype(kind)


def setup_inputs(seed: int = 0, part: int = 0) -> dict:
    streams_of = jax.random.split(jax.random.key(seed), 5)
    part_keys = jax.random.split(jax.random.fold_in(streams_of[4], part), 5)
    return {
        "pixels": bell_draw(part_keys[0], (NY, NX), 1.0, 6.0, ((0, 16),), jnp.float32),
        "row_taps": bell_draw(part_keys[1], (NX,), NX ** -0.5, 0.046875, ((0, 16),), jnp.float32),
        "column_taps": bell_draw(part_keys[2], (NY,), NY ** -0.5, 0.25, ((0, 16),), jnp.float32),
        "stencil": bell_draw(part_keys[3], (3, 3), 0.5, 3.0, (), jnp.float32),
    }


def reference(pixels, row_taps, column_taps, stencil):
    row_spectrum = jnp.fft.rfft(row_taps)
    column_spectrum = jnp.fft.rfft(column_taps)
    row_done = jnp.fft.irfft(jnp.fft.rfft(pixels, axis=1) * row_spectrum[None, :], n=NX, axis=1)
    combined = jnp.fft.irfft(jnp.fft.rfft(row_done, axis=0) * column_spectrum[:, None], n=NY, axis=0)
    filtered = combined.astype(pixels.dtype)
    for offset_row in range(3):
        for offset_col in range(3):
            moved = jnp.roll(pixels, (1 - offset_row, 1 - offset_col), axis=(0, 1))
            filtered = filtered + stencil[offset_row, offset_col] * moved
    return filtered
```

```python
import functools
import math

import jax
import jax.numpy as jnp
import numpy as np
from jax import lax
from jax.experimental import pallas as pl
from jax.experimental.pallas import tpu as pltpu
from jax.sharding import PartitionSpec as P

dft_precision = lax.Precision.HIGH
row_forms = ("kj,rjm->rkm", "rkm,ml->rkl")
column_forms = ("kj,jmc->kmc", "kmc,ml->klc")


def padded_2(cells, sides, width):
    for axis, dim in sides:
        count = lax.axis_size(axis)
        head = lax.slice_in_dim(cells, 0, width, axis=dim)
        tail = lax.slice_in_dim(cells, cells.shape[dim] - width, cells.shape[dim], axis=dim)
        cells = jnp.concatenate(
            [
                lax.ppermute(tail, axis, [(i, (i + 1) % count) for i in range(count)]),
                cells,
                lax.ppermute(head, axis, [((i + 1) % count, i) for i in range(count)]),
            ],
            axis=dim,
        )
    return cells


def split_length(length):
    factor = int(math.isqrt(length))
    while length % factor:
        factor -= 1
    return (length // factor, factor)


def dft_tables(length):
    positions = jnp.arange(length, dtype=jnp.int32)
    product = positions[:, None] * positions[None, :] % length
    angles = product.astype(jnp.float32) * (2.0 * math.pi / length)
    return (jnp.cos(angles), -jnp.sin(angles))


def prepare(length, twist_shape):
    outer_len, inner_len = split_length(length)
    cos_outer, sin_outer = dft_tables(outer_len)
    cos_inner, sin_inner = dft_tables(inner_len)
    outer_pos = jnp.arange(outer_len, dtype=jnp.int32)
    inner_pos = jnp.arange(inner_len, dtype=jnp.int32)
    product = outer_pos[:, None] * inner_pos[None, :] % length
    angles = product.astype(jnp.float32) * (2.0 * math.pi / length)
    twist_real = jnp.cos(angles).reshape(twist_shape)
    twist_imag = (-jnp.sin(angles)).reshape(twist_shape)
    return (
        outer_len,
        inner_len,
        cos_outer,
        sin_outer,
        cos_inner,
        sin_inner,
        twist_real,
        twist_imag,
    )


def contract(form, left, right):
    return jnp.einsum(
        form, left, right, precision=dft_precision, preferred_element_type=jnp.float32
    )


def forward(values, tables, forms):
    outer_len, inner_len, cos_outer, sin_outer, cos_inner, sin_inner, twist_real, twist_imag = (
        tables
    )
    first_real = contract(forms[0], cos_outer, values)
    first_imag = contract(forms[0], sin_outer, values)
    turned_real = first_real * twist_real - first_imag * twist_imag
    turned_imag = first_real * twist_imag + first_imag * twist_real
    out_real = contract(forms[1], turned_real, cos_inner) - contract(
        forms[1], turned_imag, sin_inner
    )
    out_imag = contract(forms[1], turned_real, sin_inner) + contract(
        forms[1], turned_imag, cos_inner
    )
    return (out_real, out_imag)


def inverse(spec_real, spec_imag, tables, forms):
    outer_len, inner_len, cos_outer, sin_outer, cos_inner, sin_inner, twist_real, twist_imag = (
        tables
    )
    back_real = contract(forms[1], spec_real, cos_inner) + contract(forms[1], spec_imag, sin_inner)
    back_imag = contract(forms[1], spec_imag, cos_inner) - contract(forms[1], spec_real, sin_inner)
    turned_real = back_real * twist_real + back_imag * twist_imag
    turned_imag = back_imag * twist_real - back_real * twist_imag
    result = contract(forms[0], cos_outer, turned_real) + contract(forms[0], sin_outer, turned_imag)
    return result / float(outer_len * inner_len)


def convolve(values, filter_spec, tables, forms):
    spec_real, spec_imag = forward(values, tables, forms)
    filter_real, filter_imag = filter_spec
    prod_real = spec_real * filter_real - spec_imag * filter_imag
    prod_imag = spec_real * filter_imag + spec_imag * filter_real
    return inverse(prod_real, prod_imag, tables, forms)


def body(pixels, row_taps, column_taps, stencil):
    rows_dev, row_length = pixels.shape
    devices_rows = lax.axis_size("rows")
    whole_row, whole_column = (
        lax.all_gather(row_taps, "rows", axis=0, tiled=True),
        lax.all_gather(column_taps, "rows", axis=0, tiled=True),
    )
    column_length = whole_column.shape[0]
    row_tables = prepare(row_length, (1, split_length(row_length)[0], split_length(row_length)[1]))
    column_tables = prepare(
        column_length, (split_length(column_length)[0], split_length(column_length)[1], 1)
    )
    row_filter = forward(whole_row.reshape(1, row_tables[0], row_tables[1]), row_tables, row_forms)
    column_filter = forward(
        whole_column.reshape(column_tables[0], column_tables[1], 1), column_tables, column_forms
    )
    cols_dev = row_length // devices_rows
    lane_width = min(128, cols_dev)
    groups = cols_dev // lane_width
    padded = padded_2(pixels, (("rows", 0),), 1)
    shaped = pixels.reshape(pixels.shape[0], row_tables[0], row_tables[1])
    blocks = (
        convolve(shaped, row_filter, row_tables, row_forms)
        .reshape(pixels.shape)
        .reshape(rows_dev, groups, devices_rows * lane_width)
    )
    moved = lax.all_to_all(blocks, "rows", split_axis=2, concat_axis=0, tiled=True)
    shaped = moved.reshape(column_tables[0], column_tables[1], -1)
    result = lax.all_to_all(
        convolve(shaped, column_filter, column_tables, column_forms).reshape(moved.shape),
        "rows",
        split_axis=0,
        concat_axis=2,
        tiled=True,
    )
    convolved = result.reshape(rows_dev, row_length)
    filtered = convolved
    for offset_row in range(3):
        row_band = padded[offset_row : offset_row + rows_dev]
        for offset_col in range(3):
            filtered = filtered + stencil[offset_row, offset_col] * jnp.roll(
                row_band, 1 - offset_col, axis=1
            )
    return filtered


def split_bf16(values):
    high = values.astype(jnp.bfloat16)
    low = (values - high.astype(jnp.float32)).astype(jnp.bfloat16)
    return high, low


def mm(left, right):
    return jnp.dot(left, right, preferred_element_type=jnp.float32)


def mm3(left, right):
    return mm(left[0], right[0]) + (mm(left[0], right[1]) + mm(left[1], right[0]))


def host_tables(side):
    length = side * side
    index = np.arange(side)
    product = index[:, None] * index[None, :]
    angle = 2.0 * np.pi * (product % side) / side
    cos, sin = np.cos(angle), np.sin(angle)
    table = np.block([[cos, sin], [-sin, cos]]).astype(np.float32)

    def halves(array):
        high = array.astype(jnp.bfloat16)
        low = (array - high.astype(np.float32)).astype(jnp.bfloat16)
        return high, low

    fwd_high, fwd_low = halves(table)
    inv_high, inv_low = halves(np.ascontiguousarray(table.T))
    turn = 2.0 * np.pi * product / length
    return (
        fwd_high,
        fwd_low,
        inv_high,
        inv_low,
        np.cos(turn).astype(np.float32),
        (-np.sin(turn)).astype(np.float32),
    )


def kernel(
    dims,
    pixels,
    row_taps,
    column_taps,
    stencil_in,
    tables_in,
    twists_in,
    out,
    padded,
    tables,
    twists,
    top_row,
    bottom_row,
    recv,
    part_high,
    part_low,
    ready,
    back,
    cells_by_row,
    halo_above,
    halo_below,
    all_row,
    all_column,
    circ_high,
    circ_low,
    filter_real,
    filter_imag,
    stencil,
    send_px,
    recv_px,
    send_taps,
    recv_row,
    recv_col,
    send_halo,
    recv_halo,
    send_back,
    recv_back,
    local_sem,
):
    count, rows_dev, side, pieces = dims
    groups = rows_dev // 8
    cols_dev = side * side // count
    a_dev = cols_dev // 128
    column_length = count * rows_dev
    piece_cols = cols_dev // pieces
    last = pieces - 1
    own = slice(8, 8 + rows_dev)
    me = lax.axis_index("rows")
    plane, spot = me // 4, lax.rem(me, 4)
    x, core = spot // 2, lax.rem(me, 2)
    low_half = plane < 2
    outer = (plane == 0) | (plane == 3)
    inner = jnp.logical_not(outer)
    first = jnp.where(low_half, core, 1 - core)

    def cross(step):
        turn = lax.rem(step // 4 + first, 2)
        depth = lax.rem(step // 2, 2)
        plane_to = jnp.where(low_half, 3 - depth, depth)
        return plane_to * 4 + lax.rem(x + turn, 2) * 2 + lax.rem(core + step, 2)

    def beside(step):
        plane_to = plane + 1 - 2 * lax.rem(plane, 2)
        return plane_to * 4 + lax.rem(x + step // 2, 2) * 2 + lax.rem(core + step, 2)

    def level(step):
        return plane * 4 + lax.rem(spot + 1 + step, 4)

    def peer(step):
        return lax.rem(me + step, count)

    def over_cross(start):
        @pl.loop(0, 8)
        def _(step):
            start(cross(step))

    def over_beside(start):
        @pl.loop(0, 4)
        def _(step):
            start(beside(step))

    def over_level(start):
        @pl.loop(0, 3)
        def _(step):
            start(level(step))

    def over_all(start):
        over_cross(start)
        over_beside(start)
        over_level(start)

    barrier = pltpu.get_barrier_semaphore()

    @pl.loop(1, count)
    def _(step):
        pl.semaphore_signal(barrier, inc=1, device_id={"rows": peer(step)})

    load_px = pltpu.make_async_copy(pixels, padded.at[own, :], local_sem.at[0])
    load_col = pltpu.make_async_copy(column_taps, all_column.at[me], local_sem.at[3])
    load_row = pltpu.make_async_copy(row_taps, all_row.at[me], local_sem.at[4])
    load_tables = pltpu.make_async_copy(tables_in, tables, local_sem.at[1])
    load_twists = pltpu.make_async_copy(twists_in, twists, local_sem.at[2])
    load_stencil = pltpu.make_async_copy(stencil_in, stencil, local_sem.at[5])
    load_col.start()
    load_px.start()
    load_row.start()
    load_tables.start()
    load_twists.start()
    load_stencil.start()

    def columns_of(rank, piece):
        return pl.ds(pl.multiple_of(rank * cols_dev + piece * piece_cols, 128), piece_cols)

    def all_columns_of(rank):
        return pl.ds(pl.multiple_of(rank * cols_dev, 128), cols_dev)

    def rows_of(rank):
        return pl.ds(pl.multiple_of(rank * rows_dev, 16), rows_dev)

    def px_start(piece, to):
        pltpu.make_async_remote_copy(
            src_ref=padded.at[own, columns_of(to, piece)],
            dst_ref=recv.at[piece, rows_of(me), :],
            send_sem=send_px,
            recv_sem=recv_px.at[piece],
            device_id={"rows": to},
        ).start()

    def px_all(piece):
        held = recv.at[piece, pl.ds(0, column_length - rows_dev), :]
        return pltpu.make_async_remote_copy(
            src_ref=held,
            dst_ref=held,
            send_sem=send_px,
            recv_sem=recv_px.at[piece],
            device_id={"rows": peer(1)},
        )

    def row_copy(to, source):
        return pltpu.make_async_remote_copy(
            src_ref=all_row.at[me],
            dst_ref=all_row.at[me],
            send_sem=send_taps.at[0, to],
            recv_sem=recv_row.at[source],
            device_id={"rows": to},
        )

    def col_copy(to, source):
        return pltpu.make_async_remote_copy(
            src_ref=all_column.at[me],
            dst_ref=all_column.at[me],
            send_sem=send_taps.at[1, to],
            recv_sem=recv_col.at[source],
            device_id={"rows": to},
        )

    def halo_copy(which):
        return pltpu.make_async_remote_copy(
            src_ref=(bottom_row, top_row)[which],
            dst_ref=(halo_above, halo_below)[which],
            send_sem=send_halo.at[which],
            recv_sem=recv_halo.at[which],
            device_id={"rows": peer(1 if which == 0 else count - 1)},
        )

    def cross_px(piece):
        if piece < pieces:
            over_cross(lambda to: px_start(piece, to))

    def beside_px(piece):
        if piece < pieces:
            over_beside(lambda to: px_start(piece, to))

    def level_px(piece):
        over_level(lambda to: px_start(piece, to))

    with jax.named_scope("barrier"):
        pl.semaphore_wait(barrier, count - 1)
    with jax.named_scope("loadpx"):
        load_col.wait()
        load_px.wait()

    over_all(lambda to: col_copy(to, me).start())
    cross_px(0)
    beside_px(0)
    level_px(0)

    top_row[...] = padded[8:9, :]
    bottom_row[...] = padded[7 + rows_dev : 8 + rows_dev, :]
    halo_copy(0).start()
    halo_copy(1).start()
    load_row.wait()
    over_all(lambda to: row_copy(to, me).start())

    @pl.when(outer)
    def _():
        beside_px(1)

    @pl.when(inner)
    def _():
        for piece in range(1, pieces):
            cross_px(piece)
            beside_px(piece)

    for piece in range(1, pieces):
        level_px(piece)

    for piece in range(pieces):
        recv[piece, rows_of(me), :] = padded[own, columns_of(me, piece)]
    load_tables.wait()
    load_twists.wait()
    load_stencil.wait()

    with jax.named_scope("waitcol"):

        @pl.loop(1, count)
        def _(step):
            col_copy(peer(step), peer(step)).wait_recv()

    per_block = 128 // rows_dev
    taps = jnp.concatenate([all_column[rank] for rank in range(count)], axis=0)
    held_at = lax.broadcasted_iota(jnp.int32, (rows_dev, 128), 0)
    lane = lax.broadcasted_iota(jnp.int32, (rows_dev, 128), 1)
    placed = []
    for spot_in in range(per_block):
        start = (per_block - 1 - spot_in) * rows_dev
        chosen_lane = jnp.where(lane == start + rows_dev - 1 - held_at, 1.0, 0.0)
        placed.append(
            jnp.dot(
                taps,
                chosen_lane,
                precision=lax.Precision.HIGHEST,
                preferred_element_type=jnp.float32,
            )
        )
    lines = []
    for block in reversed(range(column_length // 128)):
        total = placed[0][block * per_block : block * per_block + 1]
        for spot_in in range(1, per_block):
            rank = block * per_block + spot_in
            total = total + placed[spot_in][rank : rank + 1]
        lines.append(total)
    line = jnp.concatenate(lines, axis=1)
    line = jnp.broadcast_to(line, (128, column_length))
    for block in range(column_length // 128):
        turned = pltpu.roll(line, block * 128 + 1, 1, stride=1, stride_axis=0)
        high, low = split_bf16(turned)
        circ_high[block * 128 : block * 128 + 128, :] = high
        circ_low[block * 128 : block * 128 + 128, :] = low

    forward_table = (0, 1)
    inverse_table = (2, 3)

    def loaded(table):
        return (tables[table[0]], tables[table[1]])

    def swap(real, imag):
        return jnp.concatenate(
            [
                jnp.concatenate([real[:, :side], imag[:, :side]], axis=1),
                jnp.concatenate([real[:, side:], imag[:, side:]], axis=1),
            ],
            axis=0,
        )

    def spectrum(cells):
        first = mm3(loaded(forward_table), split_bf16(cells))
        real, imag = first[:side], first[side:]
        turn_r = jnp.concatenate([twists[0]] * 2, axis=1)
        turn_i = jnp.concatenate([twists[1]] * 2, axis=1)
        turned_cells = swap(real * turn_r - imag * turn_i, real * turn_i + imag * turn_r)
        return mm3(split_bf16(turned_cells), loaded(inverse_table))

    def inverse_of(real, imag):
        cells = jnp.concatenate([real, imag], axis=1)
        first = mm3(split_bf16(cells), loaded(forward_table))
        real, imag = first[:, :side], first[:, side:]
        turn_r = jnp.concatenate([twists[0]] * 2, axis=0)
        turn_i = jnp.concatenate([twists[1]] * 2, axis=0)
        back_real = real * turn_r + imag * turn_i
        back_imag = imag * turn_r - real * turn_i
        cells = jnp.concatenate(
            [
                jnp.concatenate([back_real[:side], back_real[side:]], axis=1),
                jnp.concatenate([back_imag[:side], back_imag[side:]], axis=1),
            ],
            axis=0,
        )
        return mm3(loaded(inverse_table), split_bf16(cells))

    def filter_spectrum():
        @pl.loop(1, count)
        def _(step):
            row_copy(peer(step), peer(step)).wait_recv()

        row_filter = jnp.concatenate([all_row[rank] for rank in range(count)], axis=0)
        nothing = jnp.zeros_like(row_filter)
        filter_spec = spectrum(
            jnp.concatenate(
                [
                    jnp.concatenate([row_filter, nothing], axis=1),
                    jnp.concatenate([nothing, nothing], axis=1),
                ],
                axis=0,
            )
        )[:side]
        filter_real[...] = filter_spec[:, :side] * (1.0 / (side * side))
        filter_imag[...] = filter_spec[:, side:] * (1.0 / (side * side))

    def add_stencil():
        halo_copy(0).wait_recv()
        halo_copy(1).wait_recv()
        padded[7:8, :] = halo_above[...]
        padded[8 + rows_dev : 9 + rows_dev, :] = halo_below[...]
        width = side * side
        for group in range(groups):
            base = group * 8
            above = padded[7 + base : 15 + base, :]
            here = padded[8 + base : 16 + base, :]
            below = padded[9 + base : 17 + base, :]
            sums = [
                stencil[0, b] * above + stencil[1, b] * here + stencil[2, b] * below
                for b in range(3)
            ]
            out[base : base + 8, :] = (
                sums[1] + pltpu.roll(sums[0], 1, 1) + pltpu.roll(sums[2], width - 1, 1)
            )

    def back_start(group, to, pieces_from, pieces_to):
        width = (pieces_to - pieces_from) * piece_cols
        at = pieces_from * piece_cols
        pltpu.make_async_remote_copy(
            src_ref=ready.at[
                pl.ds(pl.multiple_of(to * rows_dev + group * 8, 8), 8), pl.ds(at, width)
            ],
            dst_ref=back.at[
                pl.ds(group * 8, 8), pl.ds(pl.multiple_of(me * cols_dev + at, 128), width)
            ],
            send_sem=send_back,
            recv_sem=recv_back.at[group],
            device_id={"rows": to},
        ).start()

    def back_all(group):
        held = back.at[pl.ds(group * 8, 8), pl.ds(0, (count - 1) * cols_dev)]
        return pltpu.make_async_remote_copy(
            src_ref=held,
            dst_ref=held,
            send_sem=send_back,
            recv_sem=recv_back.at[group],
            device_id={"rows": peer(1)},
        )

    def rest(group):
        def start(to):
            back_start(group, to, last if group == 0 else 0, pieces)

        return start

    def early(piece):
        over_all(lambda to: back_start(0, to, piece, piece + 1))

    for piece in range(pieces):
        with jax.named_scope(f"waitpx#p={piece}"):
            px_all(piece).wait_recv()

        @pl.when(outer)
        def _(piece=piece):
            cross_px(piece + 1)
            beside_px(piece + 2)
            if piece == last:
                for sent in range(last):
                    early(sent)

        with jax.named_scope(f"mm#p={piece}"):
            high, low = split_bf16(recv[piece])
            part_high[...] = high
            part_low[...] = low
            at = slice(piece * piece_cols, (piece + 1) * piece_cols)
            ready[:, at] = mm3(
                (circ_high[...], circ_low[...]), (part_high[...], part_low[...])
            )
        if piece != last:

            @pl.when(inner)
            def _(piece=piece):
                early(piece)

        if piece == 0:
            with jax.named_scope("stencil"):
                add_stencil()
        if piece == 1:
            with jax.named_scope("filtspec"):
                filter_spectrum()

    @pl.when(outer)
    def _():
        over_cross(rest(0))
        over_beside(rest(0))
        over_beside(rest(1))

    @pl.when(inner)
    def _():
        for group in range(groups):
            over_cross(rest(group))
            over_beside(rest(group))

    for group in range(groups):
        over_level(rest(group))
    back[:, all_columns_of(me)] = ready[rows_of(me), :]

    flat_cells = cells_by_row.reshape(rows_dev * side, side)
    for group in range(groups):
        with jax.named_scope(f"waitback#g={group}"):
            back_all(group).wait_recv()

        @pl.when(outer)
        def _(group=group):
            if group + 1 < groups:
                over_cross(rest(group + 1))
            if group + 2 < groups:
                over_beside(rest(group + 2))

        with jax.named_scope(f"fft#g={group}"):
            for a in range(side):
                flat_cells[pl.ds(group * 8 * side + a, 8, stride=side), :] = back[
                    group * 8 : group * 8 + 8, a * side : (a + 1) * side
                ]
            for half in range(2):
                row = group * 8 + half * 4
                cells = jnp.concatenate(
                    [
                        jnp.concatenate([cells_by_row[row], cells_by_row[row + 2]], axis=1),
                        jnp.concatenate([cells_by_row[row + 1], cells_by_row[row + 3]], axis=1),
                    ],
                    axis=0,
                )
                spec = spectrum(cells)
                real, imag = spec[:, :side], spec[:, side:]
                filt_r = jnp.concatenate([filter_real[...]] * 2, axis=0)
                filt_i = jnp.concatenate([filter_imag[...]] * 2, axis=0)
                done = inverse_of(real * filt_r - imag * filt_i, real * filt_i + imag * filt_r)
                cells_by_row[row] = done[:side, :side]
                cells_by_row[row + 1] = done[side:, :side]
                cells_by_row[row + 2] = done[:side, side:]
                cells_by_row[row + 3] = done[side:, side:]
            for a in range(side):
                cut = slice(a * side, (a + 1) * side)
                out[group * 8 : group * 8 + 8, cut] += flat_cells[
                    pl.ds(group * 8 * side + a, 8, stride=side), :
                ]

    with jax.named_scope("drain"):
        halo_copy(0).wait_send()
        halo_copy(1).wait_send()
        for piece in range(pieces):
            px_all(piece).wait_send()
        for group in range(groups):
            back_all(group).wait_send()

        @pl.loop(1, count)
        def _(step):
            row_copy(peer(step), peer(step)).wait_send()
            col_copy(peer(step), peer(step)).wait_send()


def fits(pixels, row_taps, column_taps):
    rows_dev, row_length = pixels.shape
    count = lax.axis_size("rows")
    side = math.isqrt(row_length)
    return (
        side == 128
        and side * side == row_length
        and row_length % (count * 1024) == 0
        and rows_dev % 16 == 0
        and 128 % rows_dev == 0
        and (count * rows_dev) % 128 == 0
        and count % (128 // rows_dev) == 0
        and count == 16
    )


def fused(pixels, row_taps, column_taps, stencil):
    rows_dev, row_length = pixels.shape
    count = lax.axis_size("rows")
    side = math.isqrt(row_length)
    column_length = rows_dev * count
    cols_dev = row_length // count
    a_dev = cols_dev // 128
    groups = rows_dev // 8
    pieces = 4
    piece_cols = cols_dev // pieces
    made = host_tables(side)
    tables = jnp.asarray(np.stack(made[:4]))
    twists = jnp.asarray(np.stack(made[4:]))
    hbm = pl.BlockSpec(memory_space=pltpu.HBM)
    vmem = pl.BlockSpec(memory_space=pltpu.VMEM)
    f32, bf16 = jnp.float32, jnp.bfloat16
    dma = pltpu.SemaphoreType.DMA
    return pl.pallas_call(
        functools.partial(kernel, (count, rows_dev, side, pieces)),
        out_shape=jax.ShapeDtypeStruct(pixels.shape, f32),
        in_specs=[hbm] * 6,
        out_specs=vmem,
        scratch_shapes=[
            pltpu.VMEM((rows_dev + 16, row_length), f32),
            pltpu.VMEM(tables.shape, bf16),
            pltpu.VMEM(twists.shape, f32),
            pltpu.VMEM((1, row_length), f32),
            pltpu.VMEM((1, row_length), f32),
            pltpu.VMEM((pieces, column_length, piece_cols), f32),
            pltpu.VMEM((column_length, piece_cols), bf16),
            pltpu.VMEM((column_length, piece_cols), bf16),
            pltpu.VMEM((column_length, cols_dev), f32),
            pltpu.VMEM((rows_dev, row_length), f32),
            pltpu.VMEM((rows_dev, side, side), f32),
            pltpu.VMEM((1, row_length), f32),
            pltpu.VMEM((1, row_length), f32),
            pltpu.VMEM((count, a_dev, 128), f32),
            pltpu.VMEM((count, 1, rows_dev), f32),
            pltpu.VMEM((column_length, column_length), bf16),
            pltpu.VMEM((column_length, column_length), bf16),
            pltpu.VMEM((side, side), f32),
            pltpu.VMEM((side, side), f32),
            pltpu.SMEM((3, 3), f32),
            dma,
            dma((pieces,)),
            dma((2, count)),
            dma((count,)),
            dma((count,)),
            dma((2,)),
            dma((2,)),
            dma,
            dma((groups,)),
            dma((6,)),
        ],
        compiler_params=pltpu.CompilerParams(
            collective_id=0, has_side_effects=True, vmem_limit_bytes=32 * 1024 * 1024
        ),
    )(
        *(
            pltpu.with_memory_space_constraint(operand, pltpu.HBM)
            for operand in (
                pixels,
                row_taps.reshape(a_dev, 128),
                column_taps.reshape(1, rows_dev),
                stencil,
                tables,
                twists,
            )
        )
    )


def chosen(pixels, row_taps, column_taps, stencil):
    if fits(pixels, row_taps, column_taps):
        return fused(pixels, row_taps, column_taps, stencil)
    return body(pixels, row_taps, column_taps, stencil)


def solution(mesh):
    in_specs = (
        P(("chan", "rows"), None),
        P(("chan", "rows")),
        P(("chan", "rows")),
        P("chan", None),
    )
    out_specs = P(("chan", "rows"), None)
    return jax.shard_map(chosen, mesh=mesh, in_specs=in_specs, out_specs=out_specs, check_vma=False)
```

```python
import functools
import math

import jax
import jax.numpy as jnp
import numpy as np
from jax import lax
from jax.experimental import pallas as pl
from jax.experimental.pallas import tpu as pltpu
from jax.sharding import PartitionSpec as P

dft_precision = lax.Precision.HIGH
row_forms = ("kj,rjm->rkm", "rkm,ml->rkl")
column_forms = ("kj,jmc->kmc", "kmc,ml->klc")


def padded_2(cells, sides, width):
    for axis, dim in sides:
        count = lax.axis_size(axis)
        head = lax.slice_in_dim(cells, 0, width, axis=dim)
        tail = lax.slice_in_dim(cells, cells.shape[dim] - width, cells.shape[dim], axis=dim)
        cells = jnp.concatenate(
            [
                lax.ppermute(tail, axis, [(i, (i + 1) % count) for i in range(count)]),
                cells,
                lax.ppermute(head, axis, [((i + 1) % count, i) for i in range(count)]),
            ],
            axis=dim,
        )
    return cells


def split_length(length):
    factor = int(math.isqrt(length))
    while length % factor:
        factor -= 1
    return (length // factor, factor)


def dft_tables(length):
    positions = jnp.arange(length, dtype=jnp.int32)
    product = positions[:, None] * positions[None, :] % length
    angles = product.astype(jnp.float32) * (2.0 * math.pi / length)
    return (jnp.cos(angles), -jnp.sin(angles))


def prepare(length, twist_shape):
    outer_len, inner_len = split_length(length)
    cos_outer, sin_outer = dft_tables(outer_len)
    cos_inner, sin_inner = dft_tables(inner_len)
    outer_pos = jnp.arange(outer_len, dtype=jnp.int32)
    inner_pos = jnp.arange(inner_len, dtype=jnp.int32)
    product = outer_pos[:, None] * inner_pos[None, :] % length
    angles = product.astype(jnp.float32) * (2.0 * math.pi / length)
    twist_real = jnp.cos(angles).reshape(twist_shape)
    twist_imag = (-jnp.sin(angles)).reshape(twist_shape)
    return (
        outer_len,
        inner_len,
        cos_outer,
        sin_outer,
        cos_inner,
        sin_inner,
        twist_real,
        twist_imag,
    )


def contract(form, left, right):
    return jnp.einsum(
        form, left, right, precision=dft_precision, preferred_element_type=jnp.float32
    )


def forward(values, tables, forms):
    outer_len, inner_len, cos_outer, sin_outer, cos_inner, sin_inner, twist_real, twist_imag = (
        tables
    )
    first_real = contract(forms[0], cos_outer, values)
    first_imag = contract(forms[0], sin_outer, values)
    turned_real = first_real * twist_real - first_imag * twist_imag
    turned_imag = first_real * twist_imag + first_imag * twist_real
    out_real = contract(forms[1], turned_real, cos_inner) - contract(
        forms[1], turned_imag, sin_inner
    )
    out_imag = contract(forms[1], turned_real, sin_inner) + contract(
        forms[1], turned_imag, cos_inner
    )
    return (out_real, out_imag)


def inverse(spec_real, spec_imag, tables, forms):
    outer_len, inner_len, cos_outer, sin_outer, cos_inner, sin_inner, twist_real, twist_imag = (
        tables
    )
    back_real = contract(forms[1], spec_real, cos_inner) + contract(forms[1], spec_imag, sin_inner)
    back_imag = contract(forms[1], spec_imag, cos_inner) - contract(forms[1], spec_real, sin_inner)
    turned_real = back_real * twist_real + back_imag * twist_imag
    turned_imag = back_imag * twist_real - back_real * twist_imag
    result = contract(forms[0], cos_outer, turned_real) + contract(forms[0], sin_outer, turned_imag)
    return result / float(outer_len * inner_len)


def convolve(values, filter_spec, tables, forms):
    spec_real, spec_imag = forward(values, tables, forms)
    filter_real, filter_imag = filter_spec
    prod_real = spec_real * filter_real - spec_imag * filter_imag
    prod_imag = spec_real * filter_imag + spec_imag * filter_real
    return inverse(prod_real, prod_imag, tables, forms)


def body(pixels, row_taps, column_taps, stencil):
    rows_dev, row_length = pixels.shape
    devices_rows = lax.axis_size("rows")
    whole_row, whole_column = (
        lax.all_gather(row_taps, "rows", axis=0, tiled=True),
        lax.all_gather(column_taps, "rows", axis=0, tiled=True),
    )
    column_length = whole_column.shape[0]
    row_tables = prepare(row_length, (1, split_length(row_length)[0], split_length(row_length)[1]))
    column_tables = prepare(
        column_length, (split_length(column_length)[0], split_length(column_length)[1], 1)
    )
    row_filter = forward(whole_row.reshape(1, row_tables[0], row_tables[1]), row_tables, row_forms)
    column_filter = forward(
        whole_column.reshape(column_tables[0], column_tables[1], 1), column_tables, column_forms
    )
    cols_dev = row_length // devices_rows
    lane_width = min(128, cols_dev)
    groups = cols_dev // lane_width
    padded = padded_2(pixels, (("rows", 0),), 1)
    shaped = pixels.reshape(pixels.shape[0], row_tables[0], row_tables[1])
    blocks = (
        convolve(shaped, row_filter, row_tables, row_forms)
        .reshape(pixels.shape)
        .reshape(rows_dev, groups, devices_rows * lane_width)
    )
    moved = lax.all_to_all(blocks, "rows", split_axis=2, concat_axis=0, tiled=True)
    shaped = moved.reshape(column_tables[0], column_tables[1], -1)
    result = lax.all_to_all(
        convolve(shaped, column_filter, column_tables, column_forms).reshape(moved.shape),
        "rows",
        split_axis=0,
        concat_axis=2,
        tiled=True,
    )
    convolved = result.reshape(rows_dev, row_length)
    filtered = convolved
    for offset_row in range(3):
        row_band = padded[offset_row : offset_row + rows_dev]
        for offset_col in range(3):
            filtered = filtered + stencil[offset_row, offset_col] * jnp.roll(
                row_band, 1 - offset_col, axis=1
            )
    return filtered


def split_bf16(values):
    high = values.astype(jnp.bfloat16)
    low = (values - high.astype(jnp.float32)).astype(jnp.bfloat16)
    return high, low


def mm(left, right):
    return jnp.dot(left, right, preferred_element_type=jnp.float32)


def mm3(left, right):
    return mm(left[0], right[0]) + (mm(left[0], right[1]) + mm(left[1], right[0]))


def host_tables(side):
    length = side * side
    index = np.arange(side)
    product = index[:, None] * index[None, :]
    angle = 2.0 * np.pi * (product % side) / side
    cos, sin = np.cos(angle), np.sin(angle)
    table = np.block([[cos, sin], [-sin, cos]]).astype(np.float32)

    def halves(array):
        high = array.astype(jnp.bfloat16)
        low = (array - high.astype(np.float32)).astype(jnp.bfloat16)
        return high, low

    fwd_high, fwd_low = halves(table)
    inv_high, inv_low = halves(np.ascontiguousarray(table.T))
    turn = 2.0 * np.pi * product / length
    return (
        fwd_high,
        fwd_low,
        inv_high,
        inv_low,
        np.cos(turn).astype(np.float32),
        (-np.sin(turn)).astype(np.float32),
    )


def bands_of(rows_dev):
    whole = [(at, 8) for at in range(0, rows_dev - 8, 8)]
    return whole + [(rows_dev - 8, 4), (rows_dev - 4, 4)]


def kernel(
    dims,
    pixels,
    row_taps,
    column_taps,
    stencil_in,
    tables_in,
    twists_in,
    out,
    padded,
    tables,
    twists,
    top_row,
    bottom_row,
    recv,
    part_high,
    part_low,
    ready,
    back,
    cells_by_row,
    halo_above,
    halo_below,
    all_row,
    all_column,
    circ_high,
    circ_low,
    filter_real,
    filter_imag,
    stencil,
    send_px,
    recv_px,
    send_row,
    send_col,
    recv_row,
    recv_col,
    send_halo,
    recv_halo,
    send_back,
    recv_back,
    local_sem,
    hello,
):
    count, rows_dev, side, pieces = dims
    bands = bands_of(rows_dev)
    groups = len(bands)
    cols_dev = side * side // count
    a_dev = cols_dev // 128
    column_length = count * rows_dev
    piece_cols = cols_dev // pieces
    last = pieces - 1
    own = slice(8, 8 + rows_dev)
    me = lax.axis_index("rows")
    plane, spot = me // 4, lax.rem(me, 4)
    x, core = spot // 2, lax.rem(me, 2)
    low_half = plane < 2
    outer = (plane == 0) | (plane == 3)
    inner = jnp.logical_not(outer)
    first = jnp.where(low_half, core, 1 - core)

    def cross(step):
        turn = lax.rem(step // 2 + first, 2)
        depth = step // 4
        plane_to = jnp.where(low_half, 3 - depth, depth)
        return plane_to * 4 + lax.rem(x + turn, 2) * 2 + lax.rem(core + step, 2)

    def beside(step):
        plane_to = plane + 1 - 2 * lax.rem(plane, 2)
        return plane_to * 4 + lax.rem(x + step // 2, 2) * 2 + lax.rem(core + step, 2)

    def level(step):
        return plane * 4 + lax.rem(spot + 1 + step, 4)

    def peer(step):
        return lax.rem(me + step, count)

    def over_cross(start):
        @pl.loop(0, 8)
        def _(step):
            start(cross(step))

    def over_beside(start):
        @pl.loop(0, 4)
        def _(step):
            start(beside(step))

    def over_level(start):
        @pl.loop(0, 3)
        def _(step):
            start(level(step))

    def over_half(start):
        over_beside(start)
        over_level(start)

    def over_all(start):
        over_cross(start)
        over_beside(start)
        over_level(start)

    mirror = lax.rem(me + count // 2, count)
    barrier = pltpu.get_barrier_semaphore()

    over_level(lambda to: pl.semaphore_signal(barrier, inc=1, device_id={"rows": to}))

    @pl.loop((plane + 1) * 4, count)
    def _(to):
        pl.semaphore_signal(barrier, inc=1, device_id={"rows": to})

    def load_part(rank, at, width, sem):
        cut = pl.ds(pl.multiple_of(rank * cols_dev + at, 128), width)
        return pltpu.make_async_copy(pixels.at[:, cut], padded.at[own, cut], local_sem.at[sem])

    def loaded_px(width, sem):
        cut = pl.ds(0, count * width)
        pltpu.make_async_copy(pixels.at[:, cut], padded.at[own, cut], local_sem.at[sem]).wait()

    load_col = pltpu.make_async_copy(column_taps, all_column.at[me], local_sem.at[3])
    load_row = pltpu.make_async_copy(row_taps, all_row.at[me], local_sem.at[4])
    load_tables = pltpu.make_async_copy(tables_in, tables, local_sem.at[1])
    load_twists = pltpu.make_async_copy(twists_in, twists, local_sem.at[2])
    load_stencil = pltpu.make_async_copy(stencil_in, stencil, local_sem.at[5])
    load_col.start()

    @pl.loop(0, count)
    def _(rank):
        load_part(rank, 0, piece_cols, 0).start()

    load_row.start()

    @pl.loop(0, count)
    def _(rank):
        load_part(rank, piece_cols, cols_dev - piece_cols, 6).start()

    load_tables.start()
    load_twists.start()
    load_stencil.start()

    def columns_of(rank, piece):
        return pl.ds(pl.multiple_of(rank * cols_dev + piece * piece_cols, 128), piece_cols)

    def all_columns_of(rank):
        return pl.ds(pl.multiple_of(rank * cols_dev, 128), cols_dev)

    def rows_of(rank):
        return pl.ds(pl.multiple_of(rank * rows_dev, 16), rows_dev)

    def px_start(piece, to):
        pltpu.make_async_remote_copy(
            src_ref=padded.at[own, columns_of(to, piece)],
            dst_ref=recv.at[piece, rows_of(me), :],
            send_sem=send_px,
            recv_sem=recv_px.at[piece],
            device_id={"rows": to},
        ).start()

    def px_all(piece):
        held = recv.at[piece, pl.ds(0, column_length - rows_dev), :]
        return pltpu.make_async_remote_copy(
            src_ref=held,
            dst_ref=held,
            send_sem=send_px,
            recv_sem=recv_px.at[piece],
            device_id={"rows": peer(1)},
        )

    def row_copy(to, which):
        return pltpu.make_async_remote_copy(
            src_ref=all_row.at[me],
            dst_ref=all_row.at[me],
            send_sem=send_row,
            recv_sem=recv_row.at[which],
            device_id={"rows": to},
        )

    def row_relay(to):
        return pltpu.make_async_remote_copy(
            src_ref=all_row.at[mirror],
            dst_ref=all_row.at[mirror],
            send_sem=send_row,
            recv_sem=recv_row.at[2],
            device_id={"rows": to},
        )

    def rows_moved(amount, which):
        held = all_row.at[pl.ds(0, amount)]
        return pltpu.make_async_remote_copy(
            src_ref=held,
            dst_ref=held,
            send_sem=send_row,
            recv_sem=recv_row.at[which],
            device_id={"rows": peer(1)},
        )

    def col_copy(to):
        return pltpu.make_async_remote_copy(
            src_ref=all_column.at[me],
            dst_ref=all_column.at[me],
            send_sem=send_col,
            recv_sem=recv_col,
            device_id={"rows": to},
        )

    def cols_moved():
        held = all_column.at[pl.ds(0, count - 1)]
        return pltpu.make_async_remote_copy(
            src_ref=held,
            dst_ref=held,
            send_sem=send_col,
            recv_sem=recv_col,
            device_id={"rows": peer(1)},
        )

    def halo_copy(which):
        return pltpu.make_async_remote_copy(
            src_ref=(bottom_row, top_row)[which],
            dst_ref=(halo_above, halo_below)[which],
            send_sem=send_halo.at[which],
            recv_sem=recv_halo.at[which],
            device_id={"rows": peer(1 if which == 0 else count - 1)},
        )

    def cross_px(piece):
        if piece < pieces:
            over_cross(lambda to: px_start(piece, to))

    def beside_px(piece):
        if piece < pieces:
            over_beside(lambda to: px_start(piece, to))

    def level_px(piece):
        over_level(lambda to: px_start(piece, to))

    with jax.named_scope("barrier"):
        pl.semaphore_wait(barrier, plane * 4 + 3)

    @pl.loop(0, plane * 4)
    def _(to):
        pl.semaphore_signal(hello.at[plane], inc=1, device_id={"rows": to})

    with jax.named_scope("loadpx"):
        load_col.wait()
        loaded_px(piece_cols, 0)

    def met(other):
        @pl.when(plane < other)
        def _():
            pl.semaphore_wait(hello.at[other], 4)

    def first_out(to):
        col_copy(to).start()
        px_start(0, to)

    def first_cross(start, stop):
        @pl.loop(start, stop)
        def _(step):
            first_out(cross(step))

    with jax.named_scope("firstout"):

        @pl.when(low_half)
        def _():
            met(1)
            over_beside(first_out)
            met(2)
            first_cross(4, 8)
            met(3)
            first_cross(0, 4)

        @pl.when(jnp.logical_not(low_half))
        def _():
            first_cross(0, 8)
            met(3)
            over_beside(first_out)

        over_level(first_out)
        load_row.wait()
        row_copy(mirror, 0).start()
        loaded_px(cols_dev - piece_cols, 6)

    top_row[...] = padded[8:9, :]
    bottom_row[...] = padded[7 + rows_dev : 8 + rows_dev, :]
    halo_copy(0).start()
    halo_copy(1).start()
    over_half(lambda to: row_copy(to, 1).start())

    @pl.when(outer)
    def _():
        beside_px(1)

    @pl.when(inner)
    def _():
        for piece in range(1, pieces):
            cross_px(piece)
            beside_px(piece)

    for piece in range(1, pieces):
        level_px(piece)

    for piece in range(pieces):
        recv[piece, rows_of(me), :] = padded[own, columns_of(me, piece)]
    load_tables.wait()
    load_twists.wait()
    load_stencil.wait()

    with jax.named_scope("waitcol"):
        cols_moved().wait_recv()

    per_block = 128 // rows_dev
    taps = jnp.concatenate([all_column[rank] for rank in range(count)], axis=0)
    held_at = lax.broadcasted_iota(jnp.int32, (rows_dev, 128), 0)
    lane = lax.broadcasted_iota(jnp.int32, (rows_dev, 128), 1)
    placed = []
    for spot_in in range(per_block):
        start = (per_block - 1 - spot_in) * rows_dev
        chosen_lane = jnp.where(lane == start + rows_dev - 1 - held_at, 1.0, 0.0)
        placed.append(
            jnp.dot(
                taps,
                chosen_lane,
                precision=lax.Precision.HIGHEST,
                preferred_element_type=jnp.float32,
            )
        )
    lines = []
    for block in reversed(range(column_length // 128)):
        total = placed[0][block * per_block : block * per_block + 1]
        for spot_in in range(1, per_block):
            rank = block * per_block + spot_in
            total = total + placed[spot_in][rank : rank + 1]
        lines.append(total)
    line = jnp.concatenate(lines, axis=1)
    line = jnp.broadcast_to(line, (128, column_length))
    for block in range(column_length // 128):
        turned = pltpu.roll(line, block * 128 + 1, 1, stride=1, stride_axis=0)
        high, low = split_bf16(turned)
        circ_high[block * 128 : block * 128 + 128, :] = high
        circ_low[block * 128 : block * 128 + 128, :] = low

    forward_table = (0, 1)
    inverse_table = (2, 3)

    def loaded(table):
        return (tables[table[0]], tables[table[1]])

    def swap(real, imag):
        return jnp.concatenate(
            [
                jnp.concatenate([real[:, :side], imag[:, :side]], axis=1),
                jnp.concatenate([real[:, side:], imag[:, side:]], axis=1),
            ],
            axis=0,
        )

    def spectrum(cells):
        first = mm3(loaded(forward_table), split_bf16(cells))
        real, imag = first[:side], first[side:]
        turn_r = jnp.concatenate([twists[0]] * 2, axis=1)
        turn_i = jnp.concatenate([twists[1]] * 2, axis=1)
        turned_cells = swap(real * turn_r - imag * turn_i, real * turn_i + imag * turn_r)
        return mm3(split_bf16(turned_cells), loaded(inverse_table))

    def inverse_of(real, imag):
        cells = jnp.concatenate([real, imag], axis=1)
        first = mm3(split_bf16(cells), loaded(forward_table))
        real, imag = first[:, :side], first[:, side:]
        turn_r = jnp.concatenate([twists[0]] * 2, axis=0)
        turn_i = jnp.concatenate([twists[1]] * 2, axis=0)
        back_real = real * turn_r + imag * turn_i
        back_imag = imag * turn_r - real * turn_i
        cells = jnp.concatenate(
            [
                jnp.concatenate([back_real[:side], back_real[side:]], axis=1),
                jnp.concatenate([back_imag[:side], back_imag[side:]], axis=1),
            ],
            axis=0,
        )
        return mm3(loaded(inverse_table), split_bf16(cells))

    def filter_spectrum():
        rows_moved(count // 2 - 1, 1).wait_recv()
        rows_moved(count // 2 - 1, 2).wait_recv()
        row_filter = jnp.concatenate([all_row[rank] for rank in range(count)], axis=0)
        nothing = jnp.zeros_like(row_filter)
        filter_spec = spectrum(
            jnp.concatenate(
                [
                    jnp.concatenate([row_filter, nothing], axis=1),
                    jnp.concatenate([nothing, nothing], axis=1),
                ],
                axis=0,
            )
        )[:side]
        filter_real[...] = filter_spec[:, :side] * (1.0 / (side * side))
        filter_imag[...] = filter_spec[:, side:] * (1.0 / (side * side))

    def add_stencil():
        halo_copy(0).wait_recv()
        halo_copy(1).wait_recv()
        padded[7:8, :] = halo_above[...]
        padded[8 + rows_dev : 9 + rows_dev, :] = halo_below[...]
        width = side * side
        for group in range(rows_dev // 8):
            base = group * 8
            above = padded[7 + base : 15 + base, :]
            here = padded[8 + base : 16 + base, :]
            below = padded[9 + base : 17 + base, :]
            sums = [
                stencil[0, b] * above + stencil[1, b] * here + stencil[2, b] * below
                for b in range(3)
            ]
            out[base : base + 8, :] = (
                sums[1] + pltpu.roll(sums[0], 1, 1) + pltpu.roll(sums[2], width - 1, 1)
            )

    def back_start(group, to, pieces_from, pieces_to):
        width = (pieces_to - pieces_from) * piece_cols
        at = pieces_from * piece_cols
        row, size = bands[group]
        pltpu.make_async_remote_copy(
            src_ref=ready.at[
                pl.ds(pl.multiple_of(to * rows_dev + row, size), size), pl.ds(at, width)
            ],
            dst_ref=back.at[
                pl.ds(row, size), pl.ds(pl.multiple_of(me * cols_dev + at, 128), width)
            ],
            send_sem=send_back,
            recv_sem=recv_back.at[group],
            device_id={"rows": to},
        ).start()

    def back_all(group):
        row, size = bands[group]
        held = back.at[pl.ds(row, size), pl.ds(0, (count - 1) * cols_dev)]
        return pltpu.make_async_remote_copy(
            src_ref=held,
            dst_ref=held,
            send_sem=send_back,
            recv_sem=recv_back.at[group],
            device_id={"rows": peer(1)},
        )

    def all_sent(sem):
        held = recv.at[:, pl.ds(0, column_length - rows_dev), :]
        pltpu.make_async_remote_copy(
            src_ref=held,
            dst_ref=held,
            send_sem=sem,
            recv_sem=recv_px.at[0],
            device_id={"rows": peer(1)},
        ).wait_send()

    def rest(group):
        def start(to):
            back_start(group, to, last if group == 0 else 0, pieces)

        return start

    def early():
        over_all(lambda to: back_start(0, to, 0, last))

    for piece in range(pieces):
        with jax.named_scope(f"waitpx#p={piece}"):
            px_all(piece).wait_recv()

        @pl.when(outer)
        def _(piece=piece):
            cross_px(piece + 1)
            beside_px(piece + 2)
            if piece == last:
                early()

        with jax.named_scope(f"mm#p={piece}"):
            high, low = split_bf16(recv[piece])
            part_high[...] = high
            part_low[...] = low
            at = slice(piece * piece_cols, (piece + 1) * piece_cols)
            ready[:, at] = mm3(
                (circ_high[...], circ_low[...]), (part_high[...], part_low[...])
            )
        if piece == last - 1:

            @pl.when(inner)
            def _():
                early()

        if piece == 0:
            with jax.named_scope("stencil"):
                add_stencil()
        if piece == 1:
            with jax.named_scope("relay"):
                rows_moved(1, 0).wait_recv()
                over_half(lambda to: row_relay(to).start())
        if piece == 2:
            with jax.named_scope("filtspec"):
                filter_spectrum()

    @pl.when(outer)
    def _():
        over_cross(rest(0))
        over_beside(rest(0))
        over_beside(rest(1))

    @pl.when(inner)
    def _():
        for group in range(groups):
            over_cross(rest(group))
            over_beside(rest(group))

    for group in range(groups):
        over_level(rest(group))
    back[:, all_columns_of(me)] = ready[rows_of(me), :]

    flat_cells = cells_by_row.reshape(rows_dev * side, side)
    for group in range(groups):
        if group == 1:
            all_sent(send_px)
            rows_moved(count - 1, 0).wait_send()
            cols_moved().wait_send()
            halo_copy(0).wait_send()
            halo_copy(1).wait_send()
        with jax.named_scope(f"waitback#g={group}"):
            back_all(group).wait_recv()

        @pl.when(outer)
        def _(group=group):
            if group + 1 < groups - 2:
                over_cross(rest(group + 1))
                over_beside(rest(group + 2))
            if group == groups - 3:
                over_cross(rest(group + 1))
                over_cross(rest(group + 2))
                over_beside(rest(group + 2))

        row, size = bands[group]
        with jax.named_scope(f"fft#g={group}"):
            for a in range(side):
                flat_cells[pl.ds(row * side + a, size, stride=side), :] = back[
                    row : row + size, a * side : (a + 1) * side
                ]
            for at in range(row, row + size, 4):
                cells = jnp.concatenate(
                    [
                        jnp.concatenate([cells_by_row[at], cells_by_row[at + 2]], axis=1),
                        jnp.concatenate([cells_by_row[at + 1], cells_by_row[at + 3]], axis=1),
                    ],
                    axis=0,
                )
                spec = spectrum(cells)
                real, imag = spec[:, :side], spec[:, side:]
                filt_r = jnp.concatenate([filter_real[...]] * 2, axis=0)
                filt_i = jnp.concatenate([filter_imag[...]] * 2, axis=0)
                done = inverse_of(real * filt_r - imag * filt_i, real * filt_i + imag * filt_r)
                cells_by_row[at] = done[:side, :side]
                cells_by_row[at + 1] = done[side:, :side]
                cells_by_row[at + 2] = done[:side, side:]
                cells_by_row[at + 3] = done[side:, side:]
            if (row + size) % 8 == 0:
                base = row + size - 8
                for a in range(side):
                    cut = slice(a * side, (a + 1) * side)
                    out[base : base + 8, cut] += flat_cells[
                        pl.ds(base * side + a, 8, stride=side), :
                    ]

    with jax.named_scope("drain"):
        all_sent(send_back)


def fits(pixels, row_taps, column_taps):
    rows_dev, row_length = pixels.shape
    count = lax.axis_size("rows")
    side = math.isqrt(row_length)
    return (
        side == 128
        and side * side == row_length
        and row_length % (count * 1024) == 0
        and rows_dev % 16 == 0
        and 128 % rows_dev == 0
        and (count * rows_dev) % 128 == 0
        and count % (128 // rows_dev) == 0
        and count == 16
    )


def fused(pixels, row_taps, column_taps, stencil):
    rows_dev, row_length = pixels.shape
    count = lax.axis_size("rows")
    side = math.isqrt(row_length)
    column_length = rows_dev * count
    cols_dev = row_length // count
    a_dev = cols_dev // 128
    groups = len(bands_of(rows_dev))
    pieces = 4
    piece_cols = cols_dev // pieces
    made = host_tables(side)
    tables = jnp.asarray(np.stack(made[:4]))
    twists = jnp.asarray(np.stack(made[4:]))
    hbm = pl.BlockSpec(memory_space=pltpu.HBM)
    vmem = pl.BlockSpec(memory_space=pltpu.VMEM)
    f32, bf16 = jnp.float32, jnp.bfloat16
    dma = pltpu.SemaphoreType.DMA
    return pl.pallas_call(
        functools.partial(kernel, (count, rows_dev, side, pieces)),
        out_shape=jax.ShapeDtypeStruct(pixels.shape, f32),
        in_specs=[hbm] * 6,
        out_specs=vmem,
        scratch_shapes=[
            pltpu.VMEM((rows_dev + 16, row_length), f32),
            pltpu.VMEM(tables.shape, bf16),
            pltpu.VMEM(twists.shape, f32),
            pltpu.VMEM((1, row_length), f32),
            pltpu.VMEM((1, row_length), f32),
            pltpu.VMEM((pieces, column_length, piece_cols), f32),
            pltpu.VMEM((column_length, piece_cols), bf16),
            pltpu.VMEM((column_length, piece_cols), bf16),
            pltpu.VMEM((column_length, cols_dev), f32),
            pltpu.VMEM((rows_dev, row_length), f32),
            pltpu.VMEM((rows_dev, side, side), f32),
            pltpu.VMEM((1, row_length), f32),
            pltpu.VMEM((1, row_length), f32),
            pltpu.VMEM((count, a_dev, 128), f32),
            pltpu.VMEM((count, 1, rows_dev), f32),
            pltpu.VMEM((column_length, column_length), bf16),
            pltpu.VMEM((column_length, column_length), bf16),
            pltpu.VMEM((side, side), f32),
            pltpu.VMEM((side, side), f32),
            pltpu.SMEM((3, 3), f32),
            dma,
            dma((pieces,)),
            dma,
            dma,
            dma((3,)),
            dma,
            dma((2,)),
            dma((2,)),
            dma,
            dma((groups,)),
            dma((7,)),
            pltpu.SemaphoreType.REGULAR((4,)),
        ],
        compiler_params=pltpu.CompilerParams(
            collective_id=0, has_side_effects=True, vmem_limit_bytes=32 * 1024 * 1024
        ),
    )(
        *(
            pltpu.with_memory_space_constraint(operand, pltpu.HBM)
            for operand in (
                pixels,
                row_taps.reshape(a_dev, 128),
                column_taps.reshape(1, rows_dev),
                stencil,
                tables,
                twists,
            )
        )
    )


def chosen(pixels, row_taps, column_taps, stencil):
    if fits(pixels, row_taps, column_taps):
        return fused(pixels, row_taps, column_taps, stencil)
    return body(pixels, row_taps, column_taps, stencil)


def solution(mesh):
    in_specs = (
        P(("chan", "rows"), None),
        P(("chan", "rows")),
        P(("chan", "rows")),
        P("chan", None),
    )
    out_specs = P(("chan", "rows"), None)
    return jax.shard_map(chosen, mesh=mesh, in_specs=in_specs, out_specs=out_specs, check_vma=False)
```

```python
import functools
import math

import jax
import jax.numpy as jnp
import numpy as np
from jax import lax
from jax.experimental import pallas as pl
from jax.experimental.pallas import tpu as pltpu
from jax.sharding import PartitionSpec as P

dft_precision = lax.Precision.HIGH
row_forms = ("kj,rjm->rkm", "rkm,ml->rkl")
column_forms = ("kj,jmc->kmc", "kmc,ml->klc")


def padded_2(cells, sides, width):
    for axis, dim in sides:
        count = lax.axis_size(axis)
        head = lax.slice_in_dim(cells, 0, width, axis=dim)
        tail = lax.slice_in_dim(cells, cells.shape[dim] - width, cells.shape[dim], axis=dim)
        cells = jnp.concatenate(
            [
                lax.ppermute(tail, axis, [(i, (i + 1) % count) for i in range(count)]),
                cells,
                lax.ppermute(head, axis, [((i + 1) % count, i) for i in range(count)]),
            ],
            axis=dim,
        )
    return cells


def split_length(length):
    factor = int(math.isqrt(length))
    while length % factor:
        factor -= 1
    return (length // factor, factor)


def dft_tables(length):
    positions = jnp.arange(length, dtype=jnp.int32)
    product = positions[:, None] * positions[None, :] % length
    angles = product.astype(jnp.float32) * (2.0 * math.pi / length)
    return (jnp.cos(angles), -jnp.sin(angles))


def prepare(length, twist_shape):
    outer_len, inner_len = split_length(length)
    cos_outer, sin_outer = dft_tables(outer_len)
    cos_inner, sin_inner = dft_tables(inner_len)
    outer_pos = jnp.arange(outer_len, dtype=jnp.int32)
    inner_pos = jnp.arange(inner_len, dtype=jnp.int32)
    product = outer_pos[:, None] * inner_pos[None, :] % length
    angles = product.astype(jnp.float32) * (2.0 * math.pi / length)
    twist_real = jnp.cos(angles).reshape(twist_shape)
    twist_imag = (-jnp.sin(angles)).reshape(twist_shape)
    return (
        outer_len,
        inner_len,
        cos_outer,
        sin_outer,
        cos_inner,
        sin_inner,
        twist_real,
        twist_imag,
    )


def contract(form, left, right):
    return jnp.einsum(
        form, left, right, precision=dft_precision, preferred_element_type=jnp.float32
    )


def forward(values, tables, forms):
    outer_len, inner_len, cos_outer, sin_outer, cos_inner, sin_inner, twist_real, twist_imag = (
        tables
    )
    first_real = contract(forms[0], cos_outer, values)
    first_imag = contract(forms[0], sin_outer, values)
    turned_real = first_real * twist_real - first_imag * twist_imag
    turned_imag = first_real * twist_imag + first_imag * twist_real
    out_real = contract(forms[1], turned_real, cos_inner) - contract(
        forms[1], turned_imag, sin_inner
    )
    out_imag = contract(forms[1], turned_real, sin_inner) + contract(
        forms[1], turned_imag, cos_inner
    )
    return (out_real, out_imag)


def inverse(spec_real, spec_imag, tables, forms):
    outer_len, inner_len, cos_outer, sin_outer, cos_inner, sin_inner, twist_real, twist_imag = (
        tables
    )
    back_real = contract(forms[1], spec_real, cos_inner) + contract(forms[1], spec_imag, sin_inner)
    back_imag = contract(forms[1], spec_imag, cos_inner) - contract(forms[1], spec_real, sin_inner)
    turned_real = back_real * twist_real + back_imag * twist_imag
    turned_imag = back_imag * twist_real - back_real * twist_imag
    result = contract(forms[0], cos_outer, turned_real) + contract(forms[0], sin_outer, turned_imag)
    return result / float(outer_len * inner_len)


def convolve(values, filter_spec, tables, forms):
    spec_real, spec_imag = forward(values, tables, forms)
    filter_real, filter_imag = filter_spec
    prod_real = spec_real * filter_real - spec_imag * filter_imag
    prod_imag = spec_real * filter_imag + spec_imag * filter_real
    return inverse(prod_real, prod_imag, tables, forms)


def body(pixels, row_taps, column_taps, stencil):
    rows_dev, row_length = pixels.shape
    devices_rows = lax.axis_size("rows")
    whole_row, whole_column = (
        lax.all_gather(row_taps, "rows", axis=0, tiled=True),
        lax.all_gather(column_taps, "rows", axis=0, tiled=True),
    )
    column_length = whole_column.shape[0]
    row_tables = prepare(row_length, (1, split_length(row_length)[0], split_length(row_length)[1]))
    column_tables = prepare(
        column_length, (split_length(column_length)[0], split_length(column_length)[1], 1)
    )
    row_filter = forward(whole_row.reshape(1, row_tables[0], row_tables[1]), row_tables, row_forms)
    column_filter = forward(
        whole_column.reshape(column_tables[0], column_tables[1], 1), column_tables, column_forms
    )
    cols_dev = row_length // devices_rows
    lane_width = min(128, cols_dev)
    groups = cols_dev // lane_width
    padded = padded_2(pixels, (("rows", 0),), 1)
    shaped = pixels.reshape(pixels.shape[0], row_tables[0], row_tables[1])
    blocks = (
        convolve(shaped, row_filter, row_tables, row_forms)
        .reshape(pixels.shape)
        .reshape(rows_dev, groups, devices_rows * lane_width)
    )
    moved = lax.all_to_all(blocks, "rows", split_axis=2, concat_axis=0, tiled=True)
    shaped = moved.reshape(column_tables[0], column_tables[1], -1)
    result = lax.all_to_all(
        convolve(shaped, column_filter, column_tables, column_forms).reshape(moved.shape),
        "rows",
        split_axis=0,
        concat_axis=2,
        tiled=True,
    )
    convolved = result.reshape(rows_dev, row_length)
    filtered = convolved
    for offset_row in range(3):
        row_band = padded[offset_row : offset_row + rows_dev]
        for offset_col in range(3):
            filtered = filtered + stencil[offset_row, offset_col] * jnp.roll(
                row_band, 1 - offset_col, axis=1
            )
    return filtered


def split_bf16(values):
    high = values.astype(jnp.bfloat16)
    low = (values - high.astype(jnp.float32)).astype(jnp.bfloat16)
    return high, low


def mm(left, right):
    return jnp.dot(left, right, preferred_element_type=jnp.float32)


def mm3(left, right):
    return mm(left[0], right[0]) + (mm(left[0], right[1]) + mm(left[1], right[0]))


def host_tables(side):
    length = side * side
    index = np.arange(side)
    product = index[:, None] * index[None, :]
    angle = 2.0 * np.pi * (product % side) / side
    cos, sin = np.cos(angle), np.sin(angle)
    table = np.block([[cos, sin], [-sin, cos]]).astype(np.float32)

    def halves(array):
        high = array.astype(jnp.bfloat16)
        low = (array - high.astype(np.float32)).astype(jnp.bfloat16)
        return high, low

    fwd_high, fwd_low = halves(table)
    inv_high, inv_low = halves(np.ascontiguousarray(table.T))
    turn = 2.0 * np.pi * product / length
    return (
        fwd_high,
        fwd_low,
        inv_high,
        inv_low,
        np.cos(turn).astype(np.float32),
        (-np.sin(turn)).astype(np.float32),
    )


def bands_of(rows_dev):
    return [(at, 8) for at in range(0, rows_dev, 8)]


def cuts_of(cols_dev):
    step = cols_dev // 4
    return [(at, step) for at in range(0, cols_dev, step)]


def kernel(
    dims,
    pixels,
    row_taps,
    column_taps,
    stencil_in,
    tables_in,
    twists_in,
    out,
    padded,
    tables,
    twists,
    top_row,
    bottom_row,
    recv,
    part_high,
    part_low,
    ready,
    back,
    cells_by_row,
    halo_above,
    halo_below,
    all_row,
    all_column,
    circ_high,
    circ_low,
    filter_real,
    filter_imag,
    stencil,
    send_px,
    recv_px,
    send_row,
    send_col,
    recv_row,
    recv_col,
    send_halo,
    recv_halo,
    send_back,
    recv_back,
    local_sem,
    hello,
):
    count, rows_dev, side = dims
    bands = bands_of(rows_dev)
    groups = len(bands)
    cols_dev = side * side // count
    a_dev = cols_dev // 128
    column_length = count * rows_dev
    cuts = cuts_of(cols_dev)
    pieces = len(cuts)
    last = pieces - 1
    own = slice(8, 8 + rows_dev)
    me = lax.axis_index("rows")
    plane, spot = me // 4, lax.rem(me, 4)
    x, core = spot // 2, lax.rem(me, 2)
    low_half = plane < 2
    outer = (plane == 0) | (plane == 3)
    inner = jnp.logical_not(outer)
    first = jnp.where(low_half, core, 1 - core)

    def cross(step):
        turn = lax.rem(step // 4 + first, 2)
        depth = lax.rem(step // 2, 2)
        plane_to = jnp.where(low_half, 3 - depth, depth)
        return plane_to * 4 + lax.rem(x + turn, 2) * 2 + lax.rem(core + step, 2)

    def beside(step):
        plane_to = plane + 1 - 2 * lax.rem(plane, 2)
        return plane_to * 4 + lax.rem(x + step // 2, 2) * 2 + lax.rem(core + step, 2)

    def level(step):
        return plane * 4 + lax.rem(spot + 1 + step, 4)

    def peer(step):
        return lax.rem(me + step, count)

    def over_cross(start):
        @pl.loop(0, 8)
        def _(step):
            start(cross(step))

    def over_cross_last(start):
        @pl.loop(0, 8)
        def _(step):
            major, minor = step // 4, lax.rem(step // 2, 2)
            depth = jnp.where(low_half, minor, major)
            side_to = jnp.where(low_half, major, minor)
            plane_to = jnp.where(low_half, 2, 0) + depth
            start(plane_to * 4 + side_to * 2 + lax.rem(core + step, 2))

    def over_beside(start):
        @pl.loop(0, 4)
        def _(step):
            start(beside(step))

    def over_level(start):
        @pl.loop(0, 3)
        def _(step):
            start(level(step))

    def over_half(start):
        over_beside(start)
        over_level(start)

    def over_all(start):
        over_cross(start)
        over_beside(start)
        over_level(start)

    mirror = lax.rem(me + count // 2, count)
    barrier = pltpu.get_barrier_semaphore()

    chip = me // 2
    partner = chip * 2 + 1 - core
    pl.semaphore_signal(barrier, inc=1, device_id={"rows": partner})

    @pl.loop((chip + 1) * 2, count)
    def _(to):
        pl.semaphore_signal(barrier, inc=1, device_id={"rows": to})

    def load_part(rank, at, width, sem):
        cut = pl.ds(pl.multiple_of(rank * cols_dev + at, 128), width)
        return pltpu.make_async_copy(pixels.at[:, cut], padded.at[own, cut], local_sem.at[sem])

    def loaded_px(width, sem):
        cut = pl.ds(0, count * width)
        pltpu.make_async_copy(pixels.at[:, cut], padded.at[own, cut], local_sem.at[sem]).wait()

    load_col = pltpu.make_async_copy(column_taps, all_column.at[me], local_sem.at[3])
    load_row = pltpu.make_async_copy(row_taps, all_row.at[me], local_sem.at[4])
    load_tables = pltpu.make_async_copy(tables_in, tables, local_sem.at[1])
    load_twists = pltpu.make_async_copy(twists_in, twists, local_sem.at[2])
    load_stencil = pltpu.make_async_copy(stencil_in, stencil, local_sem.at[5])
    load_col.start()

    @pl.loop(0, count)
    def _(rank):
        load_part(rank, 0, cuts[1][0], 0).start()

    load_row.start()

    @pl.loop(0, count)
    def _(rank):
        load_part(rank, cuts[1][0], cols_dev - cuts[1][0], 6).start()

    load_tables.start()
    load_twists.start()
    load_stencil.start()

    def columns_of(rank, piece):
        at, width = cuts[piece]
        return pl.ds(pl.multiple_of(rank * cols_dev + at, 128), width)

    def all_columns_of(rank):
        return pl.ds(pl.multiple_of(rank * cols_dev, 128), cols_dev)

    def rows_of(rank):
        return pl.ds(pl.multiple_of(rank * rows_dev, 16), rows_dev)

    def px_start(piece, to):
        pltpu.make_async_remote_copy(
            src_ref=padded.at[own, columns_of(to, piece)],
            dst_ref=recv.at[rows_of(me), pl.ds(*cuts[piece])],
            send_sem=send_px,
            recv_sem=recv_px.at[piece],
            device_id={"rows": to},
        ).start()

    def px_all(piece):
        held = recv.at[pl.ds(0, column_length - rows_dev), pl.ds(*cuts[piece])]
        return pltpu.make_async_remote_copy(
            src_ref=held,
            dst_ref=held,
            send_sem=send_px,
            recv_sem=recv_px.at[piece],
            device_id={"rows": peer(1)},
        )

    def row_copy(to, which):
        return pltpu.make_async_remote_copy(
            src_ref=all_row.at[me],
            dst_ref=all_row.at[me],
            send_sem=send_row,
            recv_sem=recv_row.at[which],
            device_id={"rows": to},
        )

    def row_relay(to):
        return pltpu.make_async_remote_copy(
            src_ref=all_row.at[mirror],
            dst_ref=all_row.at[mirror],
            send_sem=send_row,
            recv_sem=recv_row.at[2],
            device_id={"rows": to},
        )

    def rows_moved(amount, which):
        held = all_row.at[pl.ds(0, amount)]
        return pltpu.make_async_remote_copy(
            src_ref=held,
            dst_ref=held,
            send_sem=send_row,
            recv_sem=recv_row.at[which],
            device_id={"rows": peer(1)},
        )

    def col_copy(to):
        return pltpu.make_async_remote_copy(
            src_ref=all_column.at[me],
            dst_ref=all_column.at[me],
            send_sem=send_col,
            recv_sem=recv_col,
            device_id={"rows": to},
        )

    def cols_moved():
        held = all_column.at[pl.ds(0, count - 1)]
        return pltpu.make_async_remote_copy(
            src_ref=held,
            dst_ref=held,
            send_sem=send_col,
            recv_sem=recv_col,
            device_id={"rows": peer(1)},
        )

    def halo_copy(which):
        return pltpu.make_async_remote_copy(
            src_ref=(bottom_row, top_row)[which],
            dst_ref=(halo_above, halo_below)[which],
            send_sem=send_halo.at[which],
            recv_sem=recv_halo.at[which],
            device_id={"rows": peer(1 if which == 0 else count - 1)},
        )

    def cross_px(piece):
        if piece < pieces:
            over_cross(lambda to: px_start(piece, to))

    def beside_px(piece):
        if piece < pieces:
            over_beside(lambda to: px_start(piece, to))

    def level_px(piece):
        over_level(lambda to: px_start(piece, to))

    with jax.named_scope("barrier"):
        pl.semaphore_wait(barrier, chip * 2 + 1)

    @pl.loop(0, chip * 2)
    def _(to):
        pl.semaphore_signal(hello.at[chip], inc=1, device_id={"rows": to})

    with jax.named_scope("loadpx"):
        load_col.wait()
        load_row.wait()
        loaded_px(cuts[1][0], 0)

    with jax.named_scope("firstout"):

        def met(other):
            @pl.when(chip < other)
            def _():
                pl.semaphore_wait(hello.at[other], 2)

        def first_out(to):
            @pl.when(to == mirror)
            def _():
                row_copy(mirror, 0).start()

            col_copy(to).start()
            px_start(0, to)

        def first_pairs(pairs, target):
            @pl.loop(0, pairs)
            def _(pair):
                to = target(pair * 2)
                met(to // 2)
                first_out(to)
                first_out(target(pair * 2 + 1))

        def risen(step):
            turn = lax.rem(step // 2 + first, 2)
            return (2 + step // 4) * 4 + lax.rem(x + turn, 2) * 2 + lax.rem(core + step, 2)

        @pl.when(low_half)
        def _():
            first_pairs(2, beside)
            first_pairs(4, risen)

        @pl.when(jnp.logical_not(low_half))
        def _():
            first_pairs(4, cross)
            first_pairs(2, beside)

        met(chip + 1 - 2 * x)
        over_level(first_out)
        loaded_px(cols_dev - cuts[1][0], 6)

    top_row[...] = padded[8:9, :]
    bottom_row[...] = padded[7 + rows_dev : 8 + rows_dev, :]
    halo_copy(0).start()
    halo_copy(1).start()
    over_half(lambda to: row_copy(to, 1).start())

    @pl.when(outer)
    def _():
        beside_px(1)

    @pl.when(inner)
    def _():
        for piece in range(1, pieces):
            cross_px(piece)
            beside_px(piece)

    for piece in range(1, pieces):
        level_px(piece)

    recv[rows_of(me), :] = padded[own, all_columns_of(me)]
    load_tables.wait()
    load_twists.wait()
    load_stencil.wait()

    with jax.named_scope("waitcol"):
        cols_moved().wait_recv()

    per_block = 128 // rows_dev
    taps = jnp.concatenate([all_column[rank] for rank in range(count)], axis=0)
    held_at = lax.broadcasted_iota(jnp.int32, (rows_dev, 128), 0)
    lane = lax.broadcasted_iota(jnp.int32, (rows_dev, 128), 1)
    placed = []
    for spot_in in range(per_block):
        start = (per_block - 1 - spot_in) * rows_dev
        chosen_lane = jnp.where(lane == start + rows_dev - 1 - held_at, 1.0, 0.0)
        placed.append(
            jnp.dot(
                taps,
                chosen_lane,
                precision=lax.Precision.HIGHEST,
                preferred_element_type=jnp.float32,
            )
        )
    lines = []
    for block in reversed(range(column_length // 128)):
        total = placed[0][block * per_block : block * per_block + 1]
        for spot_in in range(1, per_block):
            rank = block * per_block + spot_in
            total = total + placed[spot_in][rank : rank + 1]
        lines.append(total)
    line = jnp.concatenate(lines, axis=1)
    line = jnp.broadcast_to(line, (128, column_length))
    for block in range(column_length // 128):
        turned = pltpu.roll(line, block * 128 + 1, 1, stride=1, stride_axis=0)
        high, low = split_bf16(turned)
        circ_high[block * 128 : block * 128 + 128, :] = high
        circ_low[block * 128 : block * 128 + 128, :] = low

    forward_table = (0, 1)
    inverse_table = (2, 3)

    def loaded(table):
        return (tables[table[0]], tables[table[1]])

    def swap(real, imag):
        return jnp.concatenate(
            [
                jnp.concatenate([real[:, :side], imag[:, :side]], axis=1),
                jnp.concatenate([real[:, side:], imag[:, side:]], axis=1),
            ],
            axis=0,
        )

    def first_turn(cells):
        first = mm3(loaded(forward_table), split_bf16(cells))
        real, imag = first[:side], first[side:]
        turn_r = jnp.concatenate([twists[0]] * 2, axis=1)
        turn_i = jnp.concatenate([twists[1]] * 2, axis=1)
        return swap(real * turn_r - imag * turn_i, real * turn_i + imag * turn_r)

    def spectrum(cells):
        return mm3(split_bf16(first_turn(cells)), loaded(inverse_table))

    def back_turn(real, imag):
        cells = jnp.concatenate([real, imag], axis=1)
        first = mm3(split_bf16(cells), loaded(forward_table))
        real, imag = first[:, :side], first[:, side:]
        turn_r = jnp.concatenate([twists[0]] * 2, axis=0)
        turn_i = jnp.concatenate([twists[1]] * 2, axis=0)
        back_real = real * turn_r + imag * turn_i
        back_imag = imag * turn_r - real * turn_i
        return jnp.concatenate(
            [
                jnp.concatenate([back_real[:side], back_real[side:]], axis=1),
                jnp.concatenate([back_imag[:side], back_imag[side:]], axis=1),
            ],
            axis=0,
        )

    def filter_spectrum():
        rows_moved(count // 2 - 1, 1).wait_recv()
        rows_moved(count // 2 - 1, 2).wait_recv()
        row_filter = jnp.concatenate([all_row[rank] for rank in range(count)], axis=0)
        nothing = jnp.zeros_like(row_filter)
        filter_spec = spectrum(
            jnp.concatenate(
                [
                    jnp.concatenate([row_filter, nothing], axis=1),
                    jnp.concatenate([nothing, nothing], axis=1),
                ],
                axis=0,
            )
        )[:side]
        filter_real[...] = filter_spec[:, :side] * (1.0 / (side * side))
        filter_imag[...] = filter_spec[:, side:] * (1.0 / (side * side))

    def add_stencil():
        halo_copy(0).wait_recv()
        halo_copy(1).wait_recv()
        padded[7:8, :] = halo_above[...]
        padded[8 + rows_dev : 9 + rows_dev, :] = halo_below[...]
        width = side * side
        for group in range(rows_dev // 8):
            base = group * 8
            above = padded[7 + base : 15 + base, :]
            here = padded[8 + base : 16 + base, :]
            below = padded[9 + base : 17 + base, :]
            sums = [
                stencil[0, b] * above + stencil[1, b] * here + stencil[2, b] * below
                for b in range(3)
            ]
            out[base : base + 8, :] = (
                sums[1] + pltpu.roll(sums[0], 1, 1) + pltpu.roll(sums[2], width - 1, 1)
            )

    def back_start(group, to, at, width):
        row, size = bands[group]
        pltpu.make_async_remote_copy(
            src_ref=ready.at[
                pl.ds(pl.multiple_of(to * rows_dev + row, size), size), pl.ds(at, width)
            ],
            dst_ref=back.at[
                pl.ds(row, size), pl.ds(pl.multiple_of(me * cols_dev + at, 128), width)
            ],
            send_sem=send_back,
            recv_sem=recv_back.at[group],
            device_id={"rows": to},
        ).start()

    def back_all(group):
        row, size = bands[group]
        held = back.at[pl.ds(row, size), pl.ds(0, (count - 1) * cols_dev)]
        return pltpu.make_async_remote_copy(
            src_ref=held,
            dst_ref=held,
            send_sem=send_back,
            recv_sem=recv_back.at[group],
            device_id={"rows": peer(1)},
        )

    def all_sent(sem):
        held = recv.at[pl.ds(0, column_length - rows_dev), :]
        pltpu.make_async_remote_copy(
            src_ref=held,
            dst_ref=held,
            send_sem=sem,
            recv_sem=recv_px.at[0],
            device_id={"rows": peer(1)},
        ).wait_send()

    def rest(group):
        def start(to):
            at = cuts[last][0] if group == 0 else 0
            back_start(group, to, at, cols_dev - at)

        return start

    def early():
        over_all(lambda to: back_start(0, to, 0, cuts[last][0]))

    for piece in range(pieces):
        with jax.named_scope(f"waitpx#p={piece}"):
            px_all(piece).wait_recv()

        @pl.when(outer)
        def _(piece=piece):
            cross_px(piece + 1)
            beside_px(piece + 2)
            if piece == last:
                early()

        with jax.named_scope(f"mm#p={piece}"):
            at, width = cuts[piece]
            high, low = split_bf16(recv[:, at : at + width])
            part_high[:, :width] = high
            part_low[:, :width] = low
            ready[:, at : at + width] = mm3(
                (circ_high[...], circ_low[...]), (part_high[:, :width], part_low[:, :width])
            )
        if piece == last - 1:

            @pl.when(inner)
            def _():
                early()

        if piece == 0:
            with jax.named_scope("stencil"):
                add_stencil()
        if piece == 1:
            with jax.named_scope("relay"):
                rows_moved(1, 0).wait_recv()
                over_half(lambda to: row_relay(to).start())

    @pl.when(outer)
    def _():
        over_cross(rest(0))
        over_beside(rest(0))
        over_beside(rest(1))

    @pl.when(inner)
    def _():
        for group in range(groups - 1):
            over_cross(rest(group))
            over_beside(rest(group))
        over_cross_last(rest(groups - 1))
        over_beside(rest(groups - 1))

    for group in range(groups):
        over_level(rest(group))
    back[:, all_columns_of(me)] = ready[rows_of(me), :]
    with jax.named_scope("filtspec"):
        filter_spectrum()

    flat_cells = cells_by_row.reshape(rows_dev * side, side)
    for group in range(groups):
        if group == 1:
            all_sent(send_px)
            rows_moved(count - 1, 0).wait_send()
            cols_moved().wait_send()
            halo_copy(0).wait_send()
            halo_copy(1).wait_send()
        with jax.named_scope(f"waitback#g={group}"):
            back_all(group).wait_recv()

        @pl.when(outer)
        def _(group=group):
            if group + 1 < groups - 1:
                over_cross(rest(group + 1))
            if group + 1 == groups - 1:
                over_cross_last(rest(group + 1))
            if group + 2 < groups:
                over_beside(rest(group + 2))

        row, size = bands[group]
        with jax.named_scope(f"fft#g={group}"):
            for a in range(side):
                flat_cells[pl.ds(row * side + a, size, stride=side), :] = back[
                    row : row + size, a * side : (a + 1) * side
                ]
            filt_r = jnp.concatenate([filter_real[...]] * 2, axis=0)
            filt_i = jnp.concatenate([filter_imag[...]] * 2, axis=0)
            starts = range(row, row + size, 4)
            held = [
                jnp.concatenate(
                    [
                        jnp.concatenate([cells_by_row[at], cells_by_row[at + 2]], axis=1),
                        jnp.concatenate([cells_by_row[at + 1], cells_by_row[at + 3]], axis=1),
                    ],
                    axis=0,
                )
                for at in starts
            ]
            held = [first_turn(cells) for cells in held]
            held = [mm3(split_bf16(cells), loaded(inverse_table)) for cells in held]
            held = [
                (
                    spec[:, :side] * filt_r - spec[:, side:] * filt_i,
                    spec[:, :side] * filt_i + spec[:, side:] * filt_r,
                )
                for spec in held
            ]
            held = [back_turn(real, imag) for real, imag in held]
            held = [mm3(loaded(inverse_table), split_bf16(cells)) for cells in held]
            for at, done in zip(starts, held):
                cells_by_row[at] = done[:side, :side]
                cells_by_row[at + 1] = done[side:, :side]
                cells_by_row[at + 2] = done[:side, side:]
                cells_by_row[at + 3] = done[side:, side:]
            if (row + size) % 8 == 0:
                base = row + size - 8
                for a in range(side):
                    cut = slice(a * side, (a + 1) * side)
                    out[base : base + 8, cut] += flat_cells[
                        pl.ds(base * side + a, 8, stride=side), :
                    ]

    with jax.named_scope("drain"):
        all_sent(send_back)


def fits(pixels, row_taps, column_taps):
    rows_dev, row_length = pixels.shape
    count = lax.axis_size("rows")
    side = math.isqrt(row_length)
    return (
        side == 128
        and side * side == row_length
        and row_length % (count * 1024) == 0
        and rows_dev % 16 == 0
        and 128 % rows_dev == 0
        and (count * rows_dev) % 128 == 0
        and count % (128 // rows_dev) == 0
        and count == 16
    )


def fused(pixels, row_taps, column_taps, stencil):
    rows_dev, row_length = pixels.shape
    count = lax.axis_size("rows")
    side = math.isqrt(row_length)
    column_length = rows_dev * count
    cols_dev = row_length // count
    a_dev = cols_dev // 128
    groups = len(bands_of(rows_dev))
    cuts = cuts_of(cols_dev)
    pieces = len(cuts)
    made = host_tables(side)
    tables = jnp.asarray(np.stack(made[:4]))
    twists = jnp.asarray(np.stack(made[4:]))
    hbm = pl.BlockSpec(memory_space=pltpu.HBM)
    vmem = pl.BlockSpec(memory_space=pltpu.VMEM)
    f32, bf16 = jnp.float32, jnp.bfloat16
    dma = pltpu.SemaphoreType.DMA
    return pl.pallas_call(
        functools.partial(kernel, (count, rows_dev, side)),
        out_shape=jax.ShapeDtypeStruct(pixels.shape, f32),
        in_specs=[hbm] * 6,
        out_specs=vmem,
        scratch_shapes=[
            pltpu.VMEM((rows_dev + 16, row_length), f32),
            pltpu.VMEM(tables.shape, bf16),
            pltpu.VMEM(twists.shape, f32),
            pltpu.VMEM((1, row_length), f32),
            pltpu.VMEM((1, row_length), f32),
            pltpu.VMEM((column_length, cols_dev), f32),
            pltpu.VMEM((column_length, cuts[0][1]), bf16),
            pltpu.VMEM((column_length, cuts[0][1]), bf16),
            pltpu.VMEM((column_length, cols_dev), f32),
            pltpu.VMEM((rows_dev, row_length), f32),
            pltpu.VMEM((rows_dev, side, side), f32),
            pltpu.VMEM((1, row_length), f32),
            pltpu.VMEM((1, row_length), f32),
            pltpu.VMEM((count, a_dev, 128), f32),
            pltpu.VMEM((count, 1, rows_dev), f32),
            pltpu.VMEM((column_length, column_length), bf16),
            pltpu.VMEM((column_length, column_length), bf16),
            pltpu.VMEM((side, side), f32),
            pltpu.VMEM((side, side), f32),
            pltpu.SMEM((3, 3), f32),
            dma,
            dma((pieces,)),
            dma,
            dma,
            dma((3,)),
            dma,
            dma((2,)),
            dma((2,)),
            dma,
            dma((groups,)),
            dma((7,)),
            pltpu.SemaphoreType.REGULAR((count // 2,)),
        ],
        compiler_params=pltpu.CompilerParams(
            collective_id=0, has_side_effects=True, vmem_limit_bytes=32 * 1024 * 1024
        ),
    )(
        *(
            pltpu.with_memory_space_constraint(operand, pltpu.HBM)
            for operand in (
                pixels,
                row_taps.reshape(a_dev, 128),
                column_taps.reshape(1, rows_dev),
                stencil,
                tables,
                twists,
            )
        )
    )


def chosen(pixels, row_taps, column_taps, stencil):
    if fits(pixels, row_taps, column_taps):
        return fused(pixels, row_taps, column_taps, stencil)
    return body(pixels, row_taps, column_taps, stencil)


def solution(mesh):
    in_specs = (
        P(("chan", "rows"), None),
        P(("chan", "rows")),
        P(("chan", "rows")),
        P("chan", None),
    )
    out_specs = P(("chan", "rows"), None)
    return jax.shard_map(chosen, mesh=mesh, in_specs=in_specs, out_specs=out_specs, check_vma=False)
```

```python
import functools
import math

import jax
import jax.numpy as jnp
import numpy as np
from jax import lax
from jax.experimental import pallas as pl
from jax.experimental.pallas import tpu as pltpu
from jax.sharding import PartitionSpec as P

dft_precision = lax.Precision.HIGH
row_forms = ("kj,rjm->rkm", "rkm,ml->rkl")
column_forms = ("kj,jmc->kmc", "kmc,ml->klc")


def padded_2(cells, sides, width):
    for axis, dim in sides:
        count = lax.axis_size(axis)
        head = lax.slice_in_dim(cells, 0, width, axis=dim)
        tail = lax.slice_in_dim(cells, cells.shape[dim] - width, cells.shape[dim], axis=dim)
        cells = jnp.concatenate(
            [
                lax.ppermute(tail, axis, [(i, (i + 1) % count) for i in range(count)]),
                cells,
                lax.ppermute(head, axis, [((i + 1) % count, i) for i in range(count)]),
            ],
            axis=dim,
        )
    return cells


def split_length(length):
    factor = int(math.isqrt(length))
    while length % factor:
        factor -= 1
    return (length // factor, factor)


def dft_tables(length):
    positions = jnp.arange(length, dtype=jnp.int32)
    product = positions[:, None] * positions[None, :] % length
    angles = product.astype(jnp.float32) * (2.0 * math.pi / length)
    return (jnp.cos(angles), -jnp.sin(angles))


def prepare(length, twist_shape):
    outer_len, inner_len = split_length(length)
    cos_outer, sin_outer = dft_tables(outer_len)
    cos_inner, sin_inner = dft_tables(inner_len)
    outer_pos = jnp.arange(outer_len, dtype=jnp.int32)
    inner_pos = jnp.arange(inner_len, dtype=jnp.int32)
    product = outer_pos[:, None] * inner_pos[None, :] % length
    angles = product.astype(jnp.float32) * (2.0 * math.pi / length)
    twist_real = jnp.cos(angles).reshape(twist_shape)
    twist_imag = (-jnp.sin(angles)).reshape(twist_shape)
    return (
        outer_len,
        inner_len,
        cos_outer,
        sin_outer,
        cos_inner,
        sin_inner,
        twist_real,
        twist_imag,
    )


def contract(form, left, right):
    return jnp.einsum(
        form, left, right, precision=dft_precision, preferred_element_type=jnp.float32
    )


def forward(values, tables, forms):
    outer_len, inner_len, cos_outer, sin_outer, cos_inner, sin_inner, twist_real, twist_imag = (
        tables
    )
    first_real = contract(forms[0], cos_outer, values)
    first_imag = contract(forms[0], sin_outer, values)
    turned_real = first_real * twist_real - first_imag * twist_imag
    turned_imag = first_real * twist_imag + first_imag * twist_real
    out_real = contract(forms[1], turned_real, cos_inner) - contract(
        forms[1], turned_imag, sin_inner
    )
    out_imag = contract(forms[1], turned_real, sin_inner) + contract(
        forms[1], turned_imag, cos_inner
    )
    return (out_real, out_imag)


def inverse(spec_real, spec_imag, tables, forms):
    outer_len, inner_len, cos_outer, sin_outer, cos_inner, sin_inner, twist_real, twist_imag = (
        tables
    )
    back_real = contract(forms[1], spec_real, cos_inner) + contract(forms[1], spec_imag, sin_inner)
    back_imag = contract(forms[1], spec_imag, cos_inner) - contract(forms[1], spec_real, sin_inner)
    turned_real = back_real * twist_real + back_imag * twist_imag
    turned_imag = back_imag * twist_real - back_real * twist_imag
    result = contract(forms[0], cos_outer, turned_real) + contract(forms[0], sin_outer, turned_imag)
    return result / float(outer_len * inner_len)


def convolve(values, filter_spec, tables, forms):
    spec_real, spec_imag = forward(values, tables, forms)
    filter_real, filter_imag = filter_spec
    prod_real = spec_real * filter_real - spec_imag * filter_imag
    prod_imag = spec_real * filter_imag + spec_imag * filter_real
    return inverse(prod_real, prod_imag, tables, forms)


def body(pixels, row_taps, column_taps, stencil):
    rows_dev, row_length = pixels.shape
    devices_rows = lax.axis_size("rows")
    whole_row, whole_column = (
        lax.all_gather(row_taps, "rows", axis=0, tiled=True),
        lax.all_gather(column_taps, "rows", axis=0, tiled=True),
    )
    column_length = whole_column.shape[0]
    row_tables = prepare(row_length, (1, split_length(row_length)[0], split_length(row_length)[1]))
    column_tables = prepare(
        column_length, (split_length(column_length)[0], split_length(column_length)[1], 1)
    )
    row_filter = forward(whole_row.reshape(1, row_tables[0], row_tables[1]), row_tables, row_forms)
    column_filter = forward(
        whole_column.reshape(column_tables[0], column_tables[1], 1), column_tables, column_forms
    )
    cols_dev = row_length // devices_rows
    lane_width = min(128, cols_dev)
    groups = cols_dev // lane_width
    padded = padded_2(pixels, (("rows", 0),), 1)
    shaped = pixels.reshape(pixels.shape[0], row_tables[0], row_tables[1])
    blocks = (
        convolve(shaped, row_filter, row_tables, row_forms)
        .reshape(pixels.shape)
        .reshape(rows_dev, groups, devices_rows * lane_width)
    )
    moved = lax.all_to_all(blocks, "rows", split_axis=2, concat_axis=0, tiled=True)
    shaped = moved.reshape(column_tables[0], column_tables[1], -1)
    result = lax.all_to_all(
        convolve(shaped, column_filter, column_tables, column_forms).reshape(moved.shape),
        "rows",
        split_axis=0,
        concat_axis=2,
        tiled=True,
    )
    convolved = result.reshape(rows_dev, row_length)
    filtered = convolved
    for offset_row in range(3):
        row_band = padded[offset_row : offset_row + rows_dev]
        for offset_col in range(3):
            filtered = filtered + stencil[offset_row, offset_col] * jnp.roll(
                row_band, 1 - offset_col, axis=1
            )
    return filtered


def split_bf16(values):
    high = values.astype(jnp.bfloat16)
    low = (values - high.astype(jnp.float32)).astype(jnp.bfloat16)
    return high, low


def mm(left, right):
    return jnp.dot(left, right, preferred_element_type=jnp.float32)


def mm3(left, right):
    return mm(left[0], right[0]) + (mm(left[0], right[1]) + mm(left[1], right[0]))


def host_tables(side):
    length = side * side
    index = np.arange(side)
    product = index[:, None] * index[None, :]
    angle = 2.0 * np.pi * (product % side) / side
    cos, sin = np.cos(angle), np.sin(angle)
    table = np.block([[cos, sin], [-sin, cos]]).astype(np.float32)

    def halves(array):
        high = array.astype(jnp.bfloat16)
        low = (array - high.astype(np.float32)).astype(jnp.bfloat16)
        return high, low

    fwd_high, fwd_low = halves(table)
    inv_high, inv_low = halves(np.ascontiguousarray(table.T))
    turn = 2.0 * np.pi * product / length
    return (
        fwd_high,
        fwd_low,
        inv_high,
        inv_low,
        np.cos(turn).astype(np.float32),
        (-np.sin(turn)).astype(np.float32),
    )


def bands_of(rows_dev):
    return [(at, 8) for at in range(0, rows_dev, 8)]


def cuts_of(cols_dev):
    step = cols_dev // 4
    return [(at, step) for at in range(0, cols_dev, step)]


def kernel(
    dims,
    pixels,
    row_taps,
    column_taps,
    stencil_in,
    tables_in,
    twists_in,
    out,
    padded,
    tables,
    twists,
    top_row,
    bottom_row,
    recv,
    part_high,
    part_low,
    ready,
    back,
    cells_by_row,
    halo_above,
    halo_below,
    all_row,
    all_column,
    circ_high,
    circ_low,
    filter_real,
    filter_imag,
    stencil,
    send_px,
    recv_px,
    send_row,
    send_col,
    recv_row,
    recv_col,
    send_halo,
    recv_halo,
    send_back,
    recv_back,
    local_sem,
    hello,
):
    count, rows_dev, side = dims
    bands = bands_of(rows_dev)
    groups = len(bands)
    cols_dev = side * side // count
    a_dev = cols_dev // 128
    column_length = count * rows_dev
    cuts = cuts_of(cols_dev)
    pieces = len(cuts)
    last = pieces - 1
    own = slice(8, 8 + rows_dev)
    me = lax.axis_index("rows")
    plane, spot = me // 4, lax.rem(me, 4)
    x, core = spot // 2, lax.rem(me, 2)
    low_half = plane < 2
    outer = (plane == 0) | (plane == 3)
    inner = jnp.logical_not(outer)
    first = jnp.where(low_half, core, 1 - core)

    def cross(step):
        turn = lax.rem(step // 4 + first, 2)
        depth = lax.rem(step // 2, 2)
        plane_to = jnp.where(low_half, 3 - depth, depth)
        return plane_to * 4 + lax.rem(x + turn, 2) * 2 + lax.rem(core + step, 2)

    def beside(step):
        plane_to = plane + 1 - 2 * lax.rem(plane, 2)
        return plane_to * 4 + lax.rem(x + step // 2, 2) * 2 + lax.rem(core + step, 2)

    def level(step):
        return plane * 4 + lax.rem(spot + 1 + step, 4)

    def peer(step):
        return lax.rem(me + step, count)

    def over_cross(start):
        @pl.loop(0, 8)
        def _(step):
            start(cross(step))

    def over_cross_last(start):
        @pl.loop(0, 8)
        def _(step):
            major, minor = step // 4, lax.rem(step // 2, 2)
            depth = jnp.where(low_half, minor, major)
            side_to = jnp.where(low_half, major, minor)
            plane_to = jnp.where(low_half, 2, 0) + depth
            start(plane_to * 4 + side_to * 2 + lax.rem(core + step, 2))

    def over_beside(start):
        @pl.loop(0, 4)
        def _(step):
            start(beside(step))

    def over_level(start):
        @pl.loop(0, 3)
        def _(step):
            start(level(step))

    def over_half(start):
        over_beside(start)
        over_level(start)

    def over_all(start):
        over_cross(start)
        over_beside(start)
        over_level(start)

    mirror = lax.rem(me + count // 2, count)
    barrier = pltpu.get_barrier_semaphore()

    chip = me // 2
    partner = chip * 2 + 1 - core
    pl.semaphore_signal(barrier, inc=1, device_id={"rows": partner})

    @pl.loop((chip + 1) * 2, count)
    def _(to):
        pl.semaphore_signal(barrier, inc=1, device_id={"rows": to})

    def load_part(rank, at, width, sem):
        cut = pl.ds(pl.multiple_of(rank * cols_dev + at, 128), width)
        return pltpu.make_async_copy(pixels.at[:, cut], padded.at[own, cut], local_sem.at[sem])

    def loaded_px(width, sem):
        cut = pl.ds(0, count * width)
        pltpu.make_async_copy(pixels.at[:, cut], padded.at[own, cut], local_sem.at[sem]).wait()

    load_col = pltpu.make_async_copy(column_taps, all_column.at[me], local_sem.at[3])
    load_row = pltpu.make_async_copy(row_taps, all_row.at[me], local_sem.at[4])
    load_tables = pltpu.make_async_copy(tables_in, tables, local_sem.at[1])
    load_twists = pltpu.make_async_copy(twists_in, twists, local_sem.at[2])
    load_stencil = pltpu.make_async_copy(stencil_in, stencil, local_sem.at[5])
    load_col.start()

    @pl.loop(0, count)
    def _(rank):
        load_part(rank, 0, cuts[1][0], 0).start()

    load_row.start()

    def columns_of(rank, piece):
        at, width = cuts[piece]
        return pl.ds(pl.multiple_of(rank * cols_dev + at, 128), width)

    def all_columns_of(rank):
        return pl.ds(pl.multiple_of(rank * cols_dev, 128), cols_dev)

    def rows_of(rank):
        return pl.ds(pl.multiple_of(rank * rows_dev, 16), rows_dev)

    def px_start(piece, to):
        pltpu.make_async_remote_copy(
            src_ref=padded.at[own, columns_of(to, piece)],
            dst_ref=recv.at[rows_of(me), pl.ds(*cuts[piece])],
            send_sem=send_px,
            recv_sem=recv_px.at[piece],
            device_id={"rows": to},
        ).start()

    def px_all(piece):
        held = recv.at[pl.ds(0, column_length - rows_dev), pl.ds(*cuts[piece])]
        return pltpu.make_async_remote_copy(
            src_ref=held,
            dst_ref=held,
            send_sem=send_px,
            recv_sem=recv_px.at[piece],
            device_id={"rows": peer(1)},
        )

    def row_copy(to, which):
        return pltpu.make_async_remote_copy(
            src_ref=all_row.at[me],
            dst_ref=all_row.at[me],
            send_sem=send_row,
            recv_sem=recv_row.at[which],
            device_id={"rows": to},
        )

    def row_relay(to):
        return pltpu.make_async_remote_copy(
            src_ref=all_row.at[mirror],
            dst_ref=all_row.at[mirror],
            send_sem=send_row,
            recv_sem=recv_row.at[2],
            device_id={"rows": to},
        )

    def rows_moved(amount, which):
        held = all_row.at[pl.ds(0, amount)]
        return pltpu.make_async_remote_copy(
            src_ref=held,
            dst_ref=held,
            send_sem=send_row,
            recv_sem=recv_row.at[which],
            device_id={"rows": peer(1)},
        )

    def col_copy(to):
        return pltpu.make_async_remote_copy(
            src_ref=all_column.at[me],
            dst_ref=all_column.at[me],
            send_sem=send_col,
            recv_sem=recv_col,
            device_id={"rows": to},
        )

    def cols_moved():
        held = all_column.at[pl.ds(0, count - 1)]
        return pltpu.make_async_remote_copy(
            src_ref=held,
            dst_ref=held,
            send_sem=send_col,
            recv_sem=recv_col,
            device_id={"rows": peer(1)},
        )

    def halo_copy(which):
        return pltpu.make_async_remote_copy(
            src_ref=(bottom_row, top_row)[which],
            dst_ref=(halo_above, halo_below)[which],
            send_sem=send_halo.at[which],
            recv_sem=recv_halo.at[which],
            device_id={"rows": peer(1 if which == 0 else count - 1)},
        )

    def cross_px(piece):
        if piece < pieces:
            over_cross(lambda to: px_start(piece, to))

    def beside_px(piece):
        if piece < pieces:
            over_beside(lambda to: px_start(piece, to))

    def level_px(piece):
        over_level(lambda to: px_start(piece, to))

    with jax.named_scope("barrier"):
        pl.semaphore_wait(barrier, chip * 2 + 1)

    @pl.loop(0, chip * 2)
    def _(to):
        pl.semaphore_signal(hello.at[chip], inc=1, device_id={"rows": to})

    @pl.loop(0, count)
    def _(rank):
        load_part(rank, cuts[1][0], cols_dev - cuts[1][0], 6).start()

    load_tables.start()
    load_twists.start()
    load_stencil.start()

    with jax.named_scope("loadpx"):
        load_col.wait()
        load_row.wait()
        loaded_px(cuts[1][0], 0)

    with jax.named_scope("firstout"):

        def met(other):
            @pl.when(chip < other)
            def _():
                pl.semaphore_wait(hello.at[other], 2)

        def first_out(to):
            @pl.when(to == mirror)
            def _():
                row_copy(mirror, 0).start()

            col_copy(to).start()
            px_start(0, to)

        def first_pairs(pairs, target):
            @pl.loop(0, pairs)
            def _(pair):
                to = target(pair * 2)
                met(to // 2)
                first_out(to)
                first_out(target(pair * 2 + 1))

        def risen(step):
            turn = lax.rem(step // 2 + first, 2)
            return (2 + step // 4) * 4 + lax.rem(x + turn, 2) * 2 + lax.rem(core + step, 2)

        @pl.when(low_half)
        def _():
            first_pairs(2, beside)
            first_pairs(4, risen)

        @pl.when(jnp.logical_not(low_half))
        def _():
            first_pairs(4, cross)
            first_pairs(2, beside)

        met(chip + 1 - 2 * x)
        over_level(first_out)
        loaded_px(cols_dev - cuts[1][0], 6)

    top_row[...] = padded[8:9, :]
    bottom_row[...] = padded[7 + rows_dev : 8 + rows_dev, :]
    halo_copy(0).start()
    halo_copy(1).start()
    over_half(lambda to: row_copy(to, 1).start())

    @pl.when(outer)
    def _():
        beside_px(1)

    @pl.when(inner)
    def _():
        for piece in range(1, pieces):
            cross_px(piece)
            beside_px(piece)

    for piece in range(1, pieces):
        level_px(piece)

    recv[rows_of(me), :] = padded[own, all_columns_of(me)]
    load_tables.wait()
    load_twists.wait()
    load_stencil.wait()

    with jax.named_scope("waitcol"):
        cols_moved().wait_recv()

    per_block = 128 // rows_dev
    taps = jnp.concatenate([all_column[rank] for rank in range(count)], axis=0)
    held_at = lax.broadcasted_iota(jnp.int32, (rows_dev, 128), 0)
    lane = lax.broadcasted_iota(jnp.int32, (rows_dev, 128), 1)
    placed = []
    for spot_in in range(per_block):
        start = (per_block - 1 - spot_in) * rows_dev
        chosen_lane = jnp.where(lane == start + rows_dev - 1 - held_at, 1.0, 0.0)
        placed.append(
            jnp.dot(
                taps,
                chosen_lane,
                precision=lax.Precision.HIGHEST,
                preferred_element_type=jnp.float32,
            )
        )
    lines = []
    for block in reversed(range(column_length // 128)):
        total = placed[0][block * per_block : block * per_block + 1]
        for spot_in in range(1, per_block):
            rank = block * per_block + spot_in
            total = total + placed[spot_in][rank : rank + 1]
        lines.append(total)
    line = jnp.concatenate(lines, axis=1)
    line = jnp.broadcast_to(line, (128, column_length))
    for block in range(column_length // 128):
        turned = pltpu.roll(line, block * 128 + 1, 1, stride=1, stride_axis=0)
        high, low = split_bf16(turned)
        circ_high[block * 128 : block * 128 + 128, :] = high
        circ_low[block * 128 : block * 128 + 128, :] = low

    forward_table = (0, 1)
    inverse_table = (2, 3)

    def loaded(table):
        return (tables[table[0]], tables[table[1]])

    def swap(real, imag):
        return jnp.concatenate(
            [
                jnp.concatenate([real[:, :side], imag[:, :side]], axis=1),
                jnp.concatenate([real[:, side:], imag[:, side:]], axis=1),
            ],
            axis=0,
        )

    def first_turn(cells):
        first = mm3(loaded(forward_table), split_bf16(cells))
        real, imag = first[:side], first[side:]
        turn_r = jnp.concatenate([twists[0]] * 2, axis=1)
        turn_i = jnp.concatenate([twists[1]] * 2, axis=1)
        return swap(real * turn_r - imag * turn_i, real * turn_i + imag * turn_r)

    def spectrum(cells):
        return mm3(split_bf16(first_turn(cells)), loaded(inverse_table))

    def back_turn(real, imag):
        cells = jnp.concatenate([real, imag], axis=1)
        first = mm3(split_bf16(cells), loaded(forward_table))
        real, imag = first[:, :side], first[:, side:]
        turn_r = jnp.concatenate([twists[0]] * 2, axis=0)
        turn_i = jnp.concatenate([twists[1]] * 2, axis=0)
        back_real = real * turn_r + imag * turn_i
        back_imag = imag * turn_r - real * turn_i
        return jnp.concatenate(
            [
                jnp.concatenate([back_real[:side], back_real[side:]], axis=1),
                jnp.concatenate([back_imag[:side], back_imag[side:]], axis=1),
            ],
            axis=0,
        )

    def filter_spectrum():
        rows_moved(count // 2 - 1, 1).wait_recv()
        rows_moved(count // 2 - 1, 2).wait_recv()
        row_filter = jnp.concatenate([all_row[rank] for rank in range(count)], axis=0)
        nothing = jnp.zeros_like(row_filter)
        filter_spec = spectrum(
            jnp.concatenate(
                [
                    jnp.concatenate([row_filter, nothing], axis=1),
                    jnp.concatenate([nothing, nothing], axis=1),
                ],
                axis=0,
            )
        )[:side]
        filter_real[...] = filter_spec[:, :side] * (1.0 / (side * side))
        filter_imag[...] = filter_spec[:, side:] * (1.0 / (side * side))

    def add_stencil():
        halo_copy(0).wait_recv()
        halo_copy(1).wait_recv()
        padded[7:8, :] = halo_above[...]
        padded[8 + rows_dev : 9 + rows_dev, :] = halo_below[...]
        width = side * side
        for group in range(rows_dev // 8):
            base = group * 8
            above = padded[7 + base : 15 + base, :]
            here = padded[8 + base : 16 + base, :]
            below = padded[9 + base : 17 + base, :]
            sums = [
                stencil[0, b] * above + stencil[1, b] * here + stencil[2, b] * below
                for b in range(3)
            ]
            out[base : base + 8, :] = (
                sums[1] + pltpu.roll(sums[0], 1, 1) + pltpu.roll(sums[2], width - 1, 1)
            )

    def back_start(group, to, at, width):
        row, size = bands[group]
        pltpu.make_async_remote_copy(
            src_ref=ready.at[
                pl.ds(pl.multiple_of(to * rows_dev + row, size), size), pl.ds(at, width)
            ],
            dst_ref=back.at[
                pl.ds(row, size), pl.ds(pl.multiple_of(me * cols_dev + at, 128), width)
            ],
            send_sem=send_back,
            recv_sem=recv_back.at[group],
            device_id={"rows": to},
        ).start()

    def back_all(group):
        row, size = bands[group]
        held = back.at[pl.ds(row, size), pl.ds(0, (count - 1) * cols_dev)]
        return pltpu.make_async_remote_copy(
            src_ref=held,
            dst_ref=held,
            send_sem=send_back,
            recv_sem=recv_back.at[group],
            device_id={"rows": peer(1)},
        )

    def all_sent(sem):
        held = recv.at[pl.ds(0, column_length - rows_dev), :]
        pltpu.make_async_remote_copy(
            src_ref=held,
            dst_ref=held,
            send_sem=sem,
            recv_sem=recv_px.at[0],
            device_id={"rows": peer(1)},
        ).wait_send()

    def rest(group):
        def start(to):
            at = cuts[last][0] if group == 0 else 0
            back_start(group, to, at, cols_dev - at)

        return start

    def early():
        over_all(lambda to: back_start(0, to, 0, cuts[last][0]))

    for piece in range(pieces):
        with jax.named_scope(f"waitpx#p={piece}"):
            px_all(piece).wait_recv()

        @pl.when(outer)
        def _(piece=piece):
            cross_px(piece + 1)
            beside_px(piece + 2)
            if piece == last:
                early()

        with jax.named_scope(f"mm#p={piece}"):
            at, width = cuts[piece]
            high, low = split_bf16(recv[:, at : at + width])
            part_high[:, :width] = high
            part_low[:, :width] = low
            ready[:, at : at + width] = mm3(
                (circ_high[...], circ_low[...]), (part_high[:, :width], part_low[:, :width])
            )
        if piece == last - 1:

            @pl.when(inner)
            def _():
                early()

        if piece == 0:
            with jax.named_scope("stencil"):
                add_stencil()
        if piece == 1:
            with jax.named_scope("relay"):
                rows_moved(1, 0).wait_recv()
                over_half(lambda to: row_relay(to).start())

    @pl.when(outer)
    def _():
        over_cross(rest(0))
        over_beside(rest(0))
        over_beside(rest(1))

    @pl.when(inner)
    def _():
        for group in range(groups - 1):
            over_cross(rest(group))
            over_beside(rest(group))
        over_cross_last(rest(groups - 1))
        over_beside(rest(groups - 1))

    for group in range(groups):
        over_level(rest(group))
    back[:, all_columns_of(me)] = ready[rows_of(me), :]
    with jax.named_scope("filtspec"):
        filter_spectrum()

    pitch = side + 8

    def cells_of(row):
        return slice(row * pitch, row * pitch + side)

    for group in range(groups):
        if group == 1:
            all_sent(send_px)
            rows_moved(count - 1, 0).wait_send()
            cols_moved().wait_send()
            halo_copy(0).wait_send()
            halo_copy(1).wait_send()
        with jax.named_scope(f"waitback#g={group}"):
            back_all(group).wait_recv()

        @pl.when(outer)
        def _(group=group):
            if group + 1 < groups - 1:
                over_cross(rest(group + 1))
            if group + 1 == groups - 1:
                over_cross_last(rest(group + 1))
            if group + 2 < groups:
                over_beside(rest(group + 2))

        row, size = bands[group]
        with jax.named_scope(f"fft#g={group}"):
            for a in range(side):
                cells_by_row[pl.ds(row * pitch + a, size, stride=pitch), :] = back[
                    row : row + size, a * side : (a + 1) * side
                ]
            filt_r = jnp.concatenate([filter_real[...]] * 2, axis=0)
            filt_i = jnp.concatenate([filter_imag[...]] * 2, axis=0)
            starts = range(row, row + size, 4)
            held = [
                jnp.concatenate(
                    [
                        jnp.concatenate(
                            [cells_by_row[cells_of(at)], cells_by_row[cells_of(at + 2)]], axis=1
                        ),
                        jnp.concatenate(
                            [cells_by_row[cells_of(at + 1)], cells_by_row[cells_of(at + 3)]], axis=1
                        ),
                    ],
                    axis=0,
                )
                for at in starts
            ]
            held = [first_turn(cells) for cells in held]
            held = [mm3(split_bf16(cells), loaded(inverse_table)) for cells in held]
            held = [
                (
                    spec[:, :side] * filt_r - spec[:, side:] * filt_i,
                    spec[:, :side] * filt_i + spec[:, side:] * filt_r,
                )
                for spec in held
            ]
            held = [back_turn(real, imag) for real, imag in held]
            held = [mm3(loaded(inverse_table), split_bf16(cells)) for cells in held]
            for at, done in zip(starts, held):
                cells_by_row[cells_of(at)] = done[:side, :side]
                cells_by_row[cells_of(at + 1)] = done[side:, :side]
                cells_by_row[cells_of(at + 2)] = done[:side, side:]
                cells_by_row[cells_of(at + 3)] = done[side:, side:]
            if (row + size) % 8 == 0:
                base = row + size - 8
                for a in range(side):
                    cut = slice(a * side, (a + 1) * side)
                    out[base : base + 8, cut] += cells_by_row[
                        pl.ds(base * pitch + a, 8, stride=pitch), :
                    ]

    with jax.named_scope("drain"):
        all_sent(send_back)


def fits(pixels, row_taps, column_taps):
    rows_dev, row_length = pixels.shape
    count = lax.axis_size("rows")
    side = math.isqrt(row_length)
    return (
        side == 128
        and side * side == row_length
        and row_length % (count * 1024) == 0
        and rows_dev % 16 == 0
        and 128 % rows_dev == 0
        and (count * rows_dev) % 128 == 0
        and count % (128 // rows_dev) == 0
        and count == 16
    )


def fused(pixels, row_taps, column_taps, stencil):
    rows_dev, row_length = pixels.shape
    count = lax.axis_size("rows")
    side = math.isqrt(row_length)
    column_length = rows_dev * count
    cols_dev = row_length // count
    a_dev = cols_dev // 128
    groups = len(bands_of(rows_dev))
    cuts = cuts_of(cols_dev)
    pieces = len(cuts)
    made = host_tables(side)
    tables = jnp.asarray(np.stack(made[:4]))
    twists = jnp.asarray(np.stack(made[4:]))
    hbm = pl.BlockSpec(memory_space=pltpu.HBM)
    vmem = pl.BlockSpec(memory_space=pltpu.VMEM)
    f32, bf16 = jnp.float32, jnp.bfloat16
    dma = pltpu.SemaphoreType.DMA
    return pl.pallas_call(
        functools.partial(kernel, (count, rows_dev, side)),
        out_shape=jax.ShapeDtypeStruct(pixels.shape, f32),
        in_specs=[hbm] * 6,
        out_specs=vmem,
        scratch_shapes=[
            pltpu.VMEM((rows_dev + 16, row_length), f32),
            pltpu.VMEM(tables.shape, bf16),
            pltpu.VMEM(twists.shape, f32),
            pltpu.VMEM((1, row_length), f32),
            pltpu.VMEM((1, row_length), f32),
            pltpu.VMEM((column_length, cols_dev), f32),
            pltpu.VMEM((column_length, cuts[0][1]), bf16),
            pltpu.VMEM((column_length, cuts[0][1]), bf16),
            pltpu.VMEM((column_length, cols_dev), f32),
            pltpu.VMEM((rows_dev, row_length), f32),
            pltpu.VMEM((rows_dev * (side + 8), side), f32),
            pltpu.VMEM((1, row_length), f32),
            pltpu.VMEM((1, row_length), f32),
            pltpu.VMEM((count, a_dev, 128), f32),
            pltpu.VMEM((count, 1, rows_dev), f32),
            pltpu.VMEM((column_length, column_length), bf16),
            pltpu.VMEM((column_length, column_length), bf16),
            pltpu.VMEM((side, side), f32),
            pltpu.VMEM((side, side), f32),
            pltpu.SMEM((3, 3), f32),
            dma,
            dma((pieces,)),
            dma,
            dma,
            dma((3,)),
            dma,
            dma((2,)),
            dma((2,)),
            dma,
            dma((groups,)),
            dma((7,)),
            pltpu.SemaphoreType.REGULAR((count // 2,)),
        ],
        compiler_params=pltpu.CompilerParams(
            collective_id=0, has_side_effects=True, vmem_limit_bytes=32 * 1024 * 1024
        ),
    )(
        *(
            pltpu.with_memory_space_constraint(operand, pltpu.HBM)
            for operand in (
                pixels,
                row_taps.reshape(a_dev, 128),
                column_taps.reshape(1, rows_dev),
                stencil,
                tables,
                twists,
            )
        )
    )


def chosen(pixels, row_taps, column_taps, stencil):
    if fits(pixels, row_taps, column_taps):
        return fused(pixels, row_taps, column_taps, stencil)
    return body(pixels, row_taps, column_taps, stencil)


def solution(mesh):
    in_specs = (
        P(("chan", "rows"), None),
        P(("chan", "rows")),
        P(("chan", "rows")),
        P("chan", None),
    )
    out_specs = P(("chan", "rows"), None)
    return jax.shard_map(chosen, mesh=mesh, in_specs=in_specs, out_specs=out_specs, check_vma=False)
```

```python
import functools
import math

import jax
import jax.numpy as jnp
import numpy as np
from jax import lax
from jax.experimental import pallas as pl
from jax.experimental.pallas import tpu as pltpu
from jax.sharding import PartitionSpec as P

dft_precision = lax.Precision.HIGH
row_forms = ("kj,rjm->rkm", "rkm,ml->rkl")
column_forms = ("kj,jmc->kmc", "kmc,ml->klc")


def padded_2(cells, sides, width):
    for axis, dim in sides:
        count = lax.axis_size(axis)
        head = lax.slice_in_dim(cells, 0, width, axis=dim)
        tail = lax.slice_in_dim(cells, cells.shape[dim] - width, cells.shape[dim], axis=dim)
        cells = jnp.concatenate(
            [
                lax.ppermute(tail, axis, [(i, (i + 1) % count) for i in range(count)]),
                cells,
                lax.ppermute(head, axis, [((i + 1) % count, i) for i in range(count)]),
            ],
            axis=dim,
        )
    return cells


def split_length(length):
    factor = int(math.isqrt(length))
    while length % factor:
        factor -= 1
    return (length // factor, factor)


def dft_tables(length):
    positions = jnp.arange(length, dtype=jnp.int32)
    product = positions[:, None] * positions[None, :] % length
    angles = product.astype(jnp.float32) * (2.0 * math.pi / length)
    return (jnp.cos(angles), -jnp.sin(angles))


def prepare(length, twist_shape):
    outer_len, inner_len = split_length(length)
    cos_outer, sin_outer = dft_tables(outer_len)
    cos_inner, sin_inner = dft_tables(inner_len)
    outer_pos = jnp.arange(outer_len, dtype=jnp.int32)
    inner_pos = jnp.arange(inner_len, dtype=jnp.int32)
    product = outer_pos[:, None] * inner_pos[None, :] % length
    angles = product.astype(jnp.float32) * (2.0 * math.pi / length)
    twist_real = jnp.cos(angles).reshape(twist_shape)
    twist_imag = (-jnp.sin(angles)).reshape(twist_shape)
    return (
        outer_len,
        inner_len,
        cos_outer,
        sin_outer,
        cos_inner,
        sin_inner,
        twist_real,
        twist_imag,
    )


def contract(form, left, right):
    return jnp.einsum(
        form, left, right, precision=dft_precision, preferred_element_type=jnp.float32
    )


def forward(values, tables, forms):
    outer_len, inner_len, cos_outer, sin_outer, cos_inner, sin_inner, twist_real, twist_imag = (
        tables
    )
    first_real = contract(forms[0], cos_outer, values)
    first_imag = contract(forms[0], sin_outer, values)
    turned_real = first_real * twist_real - first_imag * twist_imag
    turned_imag = first_real * twist_imag + first_imag * twist_real
    out_real = contract(forms[1], turned_real, cos_inner) - contract(
        forms[1], turned_imag, sin_inner
    )
    out_imag = contract(forms[1], turned_real, sin_inner) + contract(
        forms[1], turned_imag, cos_inner
    )
    return (out_real, out_imag)


def inverse(spec_real, spec_imag, tables, forms):
    outer_len, inner_len, cos_outer, sin_outer, cos_inner, sin_inner, twist_real, twist_imag = (
        tables
    )
    back_real = contract(forms[1], spec_real, cos_inner) + contract(forms[1], spec_imag, sin_inner)
    back_imag = contract(forms[1], spec_imag, cos_inner) - contract(forms[1], spec_real, sin_inner)
    turned_real = back_real * twist_real + back_imag * twist_imag
    turned_imag = back_imag * twist_real - back_real * twist_imag
    result = contract(forms[0], cos_outer, turned_real) + contract(forms[0], sin_outer, turned_imag)
    return result / float(outer_len * inner_len)


def convolve(values, filter_spec, tables, forms):
    spec_real, spec_imag = forward(values, tables, forms)
    filter_real, filter_imag = filter_spec
    prod_real = spec_real * filter_real - spec_imag * filter_imag
    prod_imag = spec_real * filter_imag + spec_imag * filter_real
    return inverse(prod_real, prod_imag, tables, forms)


def body(pixels, row_taps, column_taps, stencil):
    rows_dev, row_length = pixels.shape
    devices_rows = lax.axis_size("rows")
    whole_row, whole_column = (
        lax.all_gather(row_taps, "rows", axis=0, tiled=True),
        lax.all_gather(column_taps, "rows", axis=0, tiled=True),
    )
    column_length = whole_column.shape[0]
    row_tables = prepare(row_length, (1, split_length(row_length)[0], split_length(row_length)[1]))
    column_tables = prepare(
        column_length, (split_length(column_length)[0], split_length(column_length)[1], 1)
    )
    row_filter = forward(whole_row.reshape(1, row_tables[0], row_tables[1]), row_tables, row_forms)
    column_filter = forward(
        whole_column.reshape(column_tables[0], column_tables[1], 1), column_tables, column_forms
    )
    cols_dev = row_length // devices_rows
    lane_width = min(128, cols_dev)
    groups = cols_dev // lane_width
    padded = padded_2(pixels, (("rows", 0),), 1)
    shaped = pixels.reshape(pixels.shape[0], row_tables[0], row_tables[1])
    blocks = (
        convolve(shaped, row_filter, row_tables, row_forms)
        .reshape(pixels.shape)
        .reshape(rows_dev, groups, devices_rows * lane_width)
    )
    moved = lax.all_to_all(blocks, "rows", split_axis=2, concat_axis=0, tiled=True)
    shaped = moved.reshape(column_tables[0], column_tables[1], -1)
    result = lax.all_to_all(
        convolve(shaped, column_filter, column_tables, column_forms).reshape(moved.shape),
        "rows",
        split_axis=0,
        concat_axis=2,
        tiled=True,
    )
    convolved = result.reshape(rows_dev, row_length)
    filtered = convolved
    for offset_row in range(3):
        row_band = padded[offset_row : offset_row + rows_dev]
        for offset_col in range(3):
            filtered = filtered + stencil[offset_row, offset_col] * jnp.roll(
                row_band, 1 - offset_col, axis=1
            )
    return filtered


def split_bf16(values):
    high = values.astype(jnp.bfloat16)
    low = (values - high.astype(jnp.float32)).astype(jnp.bfloat16)
    return high, low


def mm(left, right):
    return jnp.dot(left, right, preferred_element_type=jnp.float32)


def mm3(left, right):
    return mm(left[0], right[0]) + (mm(left[0], right[1]) + mm(left[1], right[0]))


def host_tables(side):
    length = side * side
    index = np.arange(side)
    product = index[:, None] * index[None, :]
    angle = 2.0 * np.pi * (product % side) / side
    cos, sin = np.cos(angle), np.sin(angle)
    table = np.block([[cos, sin], [-sin, cos]]).astype(np.float32)

    def halves(array):
        high = array.astype(jnp.bfloat16)
        low = (array - high.astype(np.float32)).astype(jnp.bfloat16)
        return high, low

    fwd_high, fwd_low = halves(table)
    inv_high, inv_low = halves(np.ascontiguousarray(table.T))
    turn = 2.0 * np.pi * product / length
    return (
        fwd_high,
        fwd_low,
        inv_high,
        inv_low,
        np.cos(turn).astype(np.float32),
        (-np.sin(turn)).astype(np.float32),
    )


def bands_of(rows_dev):
    return [(at, 8) for at in range(0, rows_dev, 8)]


def cuts_of(cols_dev):
    step = cols_dev // 4
    return [(at, step) for at in range(0, cols_dev, step)]


def kernel(
    dims,
    pixels,
    row_taps,
    column_taps,
    stencil_in,
    tables_in,
    twists_in,
    out,
    padded,
    tables,
    twists,
    top_row,
    bottom_row,
    recv,
    part_high,
    part_low,
    ready,
    back,
    cells_by_row,
    halo_above,
    halo_below,
    all_row,
    all_column,
    circ_high,
    circ_low,
    filter_real,
    filter_imag,
    stencil,
    send_px,
    recv_px,
    send_row,
    send_col,
    recv_row,
    recv_col,
    send_halo,
    recv_halo,
    send_back,
    recv_back,
    local_sem,
    hello,
):
    count, rows_dev, side = dims
    bands = bands_of(rows_dev)
    groups = len(bands)
    cols_dev = side * side // count
    a_dev = cols_dev // 128
    column_length = count * rows_dev
    cuts = cuts_of(cols_dev)
    pieces = len(cuts)
    last = pieces - 1
    own = slice(8, 8 + rows_dev)
    me = lax.axis_index("rows")
    plane, spot = me // 4, lax.rem(me, 4)
    x, core = spot // 2, lax.rem(me, 2)
    low_half = plane < 2
    outer = (plane == 0) | (plane == 3)
    inner = jnp.logical_not(outer)
    first = jnp.where(low_half, core, 1 - core)

    def cross(step):
        turn = lax.rem(step // 4 + first, 2)
        depth = lax.rem(step // 2, 2)
        plane_to = jnp.where(low_half, 3 - depth, depth)
        return plane_to * 4 + lax.rem(x + turn, 2) * 2 + lax.rem(core + step, 2)

    def beside(step):
        plane_to = plane + 1 - 2 * lax.rem(plane, 2)
        return plane_to * 4 + lax.rem(x + step // 2, 2) * 2 + lax.rem(core + step, 2)

    def level(step):
        return plane * 4 + lax.rem(spot + 1 + step, 4)

    def peer(step):
        return lax.rem(me + step, count)

    def over_cross(start):
        @pl.loop(0, 8)
        def _(step):
            start(cross(step))

    def over_cross_last(start):
        @pl.loop(0, 8)
        def _(step):
            major, minor = step // 4, lax.rem(step // 2, 2)
            depth = jnp.where(low_half, minor, major)
            side_to = jnp.where(low_half, major, minor)
            plane_to = jnp.where(low_half, 2, 0) + depth
            start(plane_to * 4 + side_to * 2 + lax.rem(core + step, 2))

    def over_beside(start):
        @pl.loop(0, 4)
        def _(step):
            start(beside(step))

    def over_level(start):
        @pl.loop(0, 3)
        def _(step):
            start(level(step))

    def over_half(start):
        over_beside(start)
        over_level(start)

    def over_all(start):
        over_cross(start)
        over_beside(start)
        over_level(start)

    mirror = lax.rem(me + count // 2, count)
    barrier = pltpu.get_barrier_semaphore()

    chip = me // 2
    partner = chip * 2 + 1 - core
    pl.semaphore_signal(barrier, inc=1, device_id={"rows": partner})

    @pl.loop((chip + 1) * 2, count)
    def _(to):
        pl.semaphore_signal(barrier, inc=1, device_id={"rows": to})

    def load_part(rank, at, width, sem):
        cut = pl.ds(pl.multiple_of(rank * cols_dev + at, 128), width)
        return pltpu.make_async_copy(pixels.at[:, cut], padded.at[own, cut], local_sem.at[sem])

    def loaded_px(width, sem):
        cut = pl.ds(0, count * width)
        pltpu.make_async_copy(pixels.at[:, cut], padded.at[own, cut], local_sem.at[sem]).wait()

    load_col = pltpu.make_async_copy(column_taps, all_column.at[me], local_sem.at[3])
    load_row = pltpu.make_async_copy(row_taps, all_row.at[me], local_sem.at[4])
    load_tables = pltpu.make_async_copy(tables_in, tables, local_sem.at[1])
    load_twists = pltpu.make_async_copy(twists_in, twists, local_sem.at[2])
    load_stencil = pltpu.make_async_copy(stencil_in, stencil, local_sem.at[5])
    load_col.start()

    @pl.loop(0, count)
    def _(rank):
        load_part(rank, 0, cuts[1][0], 0).start()

    load_row.start()

    def columns_of(rank, piece):
        at, width = cuts[piece]
        return pl.ds(pl.multiple_of(rank * cols_dev + at, 128), width)

    def all_columns_of(rank):
        return pl.ds(pl.multiple_of(rank * cols_dev, 128), cols_dev)

    def rows_of(rank):
        return pl.ds(pl.multiple_of(rank * rows_dev, 16), rows_dev)

    def px_start(piece, to):
        pltpu.make_async_remote_copy(
            src_ref=padded.at[own, columns_of(to, piece)],
            dst_ref=recv.at[rows_of(me), pl.ds(*cuts[piece])],
            send_sem=send_px,
            recv_sem=recv_px.at[piece],
            device_id={"rows": to},
        ).start()

    def px_all(piece):
        held = recv.at[pl.ds(0, column_length - rows_dev), pl.ds(*cuts[piece])]
        return pltpu.make_async_remote_copy(
            src_ref=held,
            dst_ref=held,
            send_sem=send_px,
            recv_sem=recv_px.at[piece],
            device_id={"rows": peer(1)},
        )

    def row_copy(to, which):
        return pltpu.make_async_remote_copy(
            src_ref=all_row.at[me],
            dst_ref=all_row.at[me],
            send_sem=send_row,
            recv_sem=recv_row.at[which],
            device_id={"rows": to},
        )

    def row_relay(to):
        return pltpu.make_async_remote_copy(
            src_ref=all_row.at[mirror],
            dst_ref=all_row.at[mirror],
            send_sem=send_row,
            recv_sem=recv_row.at[2],
            device_id={"rows": to},
        )

    def rows_moved(amount, which):
        held = all_row.at[pl.ds(0, amount)]
        return pltpu.make_async_remote_copy(
            src_ref=held,
            dst_ref=held,
            send_sem=send_row,
            recv_sem=recv_row.at[which],
            device_id={"rows": peer(1)},
        )

    def col_copy(to):
        return pltpu.make_async_remote_copy(
            src_ref=all_column.at[me],
            dst_ref=all_column.at[me],
            send_sem=send_col,
            recv_sem=recv_col,
            device_id={"rows": to},
        )

    def cols_moved():
        held = all_column.at[pl.ds(0, count - 1)]
        return pltpu.make_async_remote_copy(
            src_ref=held,
            dst_ref=held,
            send_sem=send_col,
            recv_sem=recv_col,
            device_id={"rows": peer(1)},
        )

    def halo_copy(which):
        return pltpu.make_async_remote_copy(
            src_ref=(bottom_row, top_row)[which],
            dst_ref=(halo_above, halo_below)[which],
            send_sem=send_halo.at[which],
            recv_sem=recv_halo.at[which],
            device_id={"rows": peer(1 if which == 0 else count - 1)},
        )

    def cross_px(piece):
        if piece < pieces:
            over_cross(lambda to: px_start(piece, to))

    def beside_px(piece):
        if piece < pieces:
            over_beside(lambda to: px_start(piece, to))

    def level_px(piece):
        over_level(lambda to: px_start(piece, to))

    with jax.named_scope("barrier"):
        pl.semaphore_wait(barrier, chip * 2 + 1)

    @pl.loop(0, chip * 2)
    def _(to):
        pl.semaphore_signal(hello.at[chip], inc=1, device_id={"rows": to})

    @pl.loop(0, count)
    def _(rank):
        load_part(rank, cuts[1][0], cols_dev - cuts[1][0], 6).start()

    load_tables.start()
    load_twists.start()
    load_stencil.start()

    with jax.named_scope("loadpx"):
        load_col.wait()
        load_row.wait()
        loaded_px(cuts[1][0], 0)

    with jax.named_scope("firstout"):

        def met(other):
            @pl.when(chip < other)
            def _():
                pl.semaphore_wait(hello.at[other], 2)

        def first_out(to):
            @pl.when(to == mirror)
            def _():
                row_copy(mirror, 0).start()

            col_copy(to).start()
            px_start(0, to)

        def first_pairs(pairs, target):
            @pl.loop(0, pairs)
            def _(pair):
                to = target(pair * 2)
                met(to // 2)
                first_out(to)
                first_out(target(pair * 2 + 1))

        def risen(step):
            turn = lax.rem(step // 2 + first, 2)
            return (2 + step // 4) * 4 + lax.rem(x + turn, 2) * 2 + lax.rem(core + step, 2)

        @pl.when(low_half)
        def _():
            first_pairs(2, beside)
            first_pairs(4, risen)

        @pl.when(jnp.logical_not(low_half))
        def _():
            first_pairs(4, cross)
            first_pairs(2, beside)

        met(chip + 1 - 2 * x)
        over_level(first_out)
        loaded_px(cols_dev - cuts[1][0], 6)

    top_row[...] = padded[8:9, :]
    bottom_row[...] = padded[7 + rows_dev : 8 + rows_dev, :]
    halo_copy(0).start()
    halo_copy(1).start()
    over_half(lambda to: row_copy(to, 1).start())

    @pl.when(outer)
    def _():
        beside_px(1)

    @pl.when(inner)
    def _():
        for piece in range(1, pieces):
            cross_px(piece)
            beside_px(piece)

    for piece in range(1, pieces):
        level_px(piece)

    recv[rows_of(me), :] = padded[own, all_columns_of(me)]
    load_tables.wait()
    load_twists.wait()
    load_stencil.wait()

    with jax.named_scope("waitcol"):
        cols_moved().wait_recv()

    per_block = 128 // rows_dev
    taps = jnp.concatenate([all_column[rank] for rank in range(count)], axis=0)
    held_at = lax.broadcasted_iota(jnp.int32, (rows_dev, 128), 0)
    lane = lax.broadcasted_iota(jnp.int32, (rows_dev, 128), 1)
    placed = []
    for spot_in in range(per_block):
        start = (per_block - 1 - spot_in) * rows_dev
        chosen_lane = jnp.where(lane == start + rows_dev - 1 - held_at, 1.0, 0.0)
        placed.append(
            jnp.dot(
                taps,
                chosen_lane,
                precision=lax.Precision.HIGHEST,
                preferred_element_type=jnp.float32,
            )
        )
    lines = []
    for block in reversed(range(column_length // 128)):
        total = placed[0][block * per_block : block * per_block + 1]
        for spot_in in range(1, per_block):
            rank = block * per_block + spot_in
            total = total + placed[spot_in][rank : rank + 1]
        lines.append(total)
    line = jnp.concatenate(lines, axis=1)
    line = jnp.broadcast_to(line, (128, column_length))
    for block in range(column_length // 128):
        turned = pltpu.roll(line, block * 128 + 1, 1, stride=1, stride_axis=0)
        high, low = split_bf16(turned)
        circ_high[block * 128 : block * 128 + 128, :] = high
        circ_low[block * 128 : block * 128 + 128, :] = low

    forward_table = (0, 1)
    inverse_table = (2, 3)

    def loaded(table):
        return (tables[table[0]], tables[table[1]])

    def swap(real, imag):
        return jnp.concatenate(
            [
                jnp.concatenate([real[:, :side], imag[:, :side]], axis=1),
                jnp.concatenate([real[:, side:], imag[:, side:]], axis=1),
            ],
            axis=0,
        )

    def first_turn(cells):
        first = mm3(loaded(forward_table), split_bf16(cells))
        real, imag = first[:side], first[side:]
        turn_r = jnp.concatenate([twists[0]] * 2, axis=1)
        turn_i = jnp.concatenate([twists[1]] * 2, axis=1)
        return swap(real * turn_r - imag * turn_i, real * turn_i + imag * turn_r)

    def spectrum(cells):
        return mm3(split_bf16(first_turn(cells)), loaded(inverse_table))

    def back_turn(real, imag):
        cells = jnp.concatenate([real, imag], axis=1)
        first = mm3(split_bf16(cells), loaded(forward_table))
        real, imag = first[:, :side], first[:, side:]
        turn_r = jnp.concatenate([twists[0]] * 2, axis=0)
        turn_i = jnp.concatenate([twists[1]] * 2, axis=0)
        back_real = real * turn_r + imag * turn_i
        back_imag = imag * turn_r - real * turn_i
        return jnp.concatenate(
            [
                jnp.concatenate([back_real[:side], back_real[side:]], axis=1),
                jnp.concatenate([back_imag[:side], back_imag[side:]], axis=1),
            ],
            axis=0,
        )

    def filter_spectrum():
        rows_moved(count // 2 - 1, 1).wait_recv()
        rows_moved(count // 2 - 1, 2).wait_recv()
        row_filter = jnp.concatenate([all_row[rank] for rank in range(count)], axis=0)
        nothing = jnp.zeros_like(row_filter)
        filter_spec = spectrum(
            jnp.concatenate(
                [
                    jnp.concatenate([row_filter, nothing], axis=1),
                    jnp.concatenate([nothing, nothing], axis=1),
                ],
                axis=0,
            )
        )[:side]
        filter_real[...] = filter_spec[:, :side] * (1.0 / (side * side))
        filter_imag[...] = filter_spec[:, side:] * (1.0 / (side * side))

    def add_stencil():
        halo_copy(0).wait_recv()
        halo_copy(1).wait_recv()
        padded[7:8, :] = halo_above[...]
        padded[8 + rows_dev : 9 + rows_dev, :] = halo_below[...]
        width = side * side
        for group in range(rows_dev // 8):
            base = group * 8
            above = padded[7 + base : 15 + base, :]
            here = padded[8 + base : 16 + base, :]
            below = padded[9 + base : 17 + base, :]
            sums = [
                stencil[0, b] * above + stencil[1, b] * here + stencil[2, b] * below
                for b in range(3)
            ]
            out[base : base + 8, :] = (
                sums[1] + pltpu.roll(sums[0], 1, 1) + pltpu.roll(sums[2], width - 1, 1)
            )

    def back_start(group, to, at, width):
        row, size = bands[group]
        pltpu.make_async_remote_copy(
            src_ref=ready.at[
                pl.ds(pl.multiple_of(to * rows_dev + row, size), size), pl.ds(at, width)
            ],
            dst_ref=back.at[
                pl.ds(row, size), pl.ds(pl.multiple_of(me * cols_dev + at, 128), width)
            ],
            send_sem=send_back,
            recv_sem=recv_back.at[group],
            device_id={"rows": to},
        ).start()

    def back_all(group):
        row, size = bands[group]
        held = back.at[pl.ds(row, size), pl.ds(0, (count - 1) * cols_dev)]
        return pltpu.make_async_remote_copy(
            src_ref=held,
            dst_ref=held,
            send_sem=send_back,
            recv_sem=recv_back.at[group],
            device_id={"rows": peer(1)},
        )

    def all_sent(sem):
        held = recv.at[pl.ds(0, column_length - rows_dev), :]
        pltpu.make_async_remote_copy(
            src_ref=held,
            dst_ref=held,
            send_sem=sem,
            recv_sem=recv_px.at[0],
            device_id={"rows": peer(1)},
        ).wait_send()

    def rest(group):
        def start(to):
            at = cuts[last][0] if group == 0 else 0
            back_start(group, to, at, cols_dev - at)

        return start

    def early():
        over_all(lambda to: back_start(0, to, 0, cuts[last][0]))

    for piece in range(pieces):
        with jax.named_scope(f"waitpx#p={piece}"):
            px_all(piece).wait_recv()

        @pl.when(outer)
        def _(piece=piece):
            if piece != last - 1:
                cross_px(piece + 1)
            if piece == last - 2:
                cross_px(last)
            beside_px(piece + 2)
            if piece == last:
                early()

        with jax.named_scope(f"mm#p={piece}"):
            at, width = cuts[piece]
            high, low = split_bf16(recv[:, at : at + width])
            part_high[:, :width] = high
            part_low[:, :width] = low
            ready[:, at : at + width] = mm3(
                (circ_high[...], circ_low[...]), (part_high[:, :width], part_low[:, :width])
            )
        if piece == last - 1:

            @pl.when(inner)
            def _():
                early()

        if piece == 0:
            with jax.named_scope("stencil"):
                add_stencil()
        if piece == 1:
            with jax.named_scope("relay"):
                rows_moved(1, 0).wait_recv()
                over_half(lambda to: row_relay(to).start())

    @pl.when(outer)
    def _():
        over_cross(rest(0))
        over_beside(rest(0))
        over_beside(rest(1))

    @pl.when(inner)
    def _():
        for group in range(groups - 1):
            over_cross(rest(group))
            over_beside(rest(group))
        over_cross_last(rest(groups - 1))
        over_beside(rest(groups - 1))

    for group in range(groups):
        over_level(rest(group))
    back[:, all_columns_of(me)] = ready[rows_of(me), :]
    with jax.named_scope("filtspec"):
        filter_spectrum()

    pitch = side + 8

    def cells_of(row):
        return slice(row * pitch, row * pitch + side)

    for group in range(groups):
        if group == 1:
            all_sent(send_px)
            rows_moved(count - 1, 0).wait_send()
            cols_moved().wait_send()
            halo_copy(0).wait_send()
            halo_copy(1).wait_send()
        with jax.named_scope(f"waitback#g={group}"):
            back_all(group).wait_recv()

        @pl.when(outer)
        def _(group=group):
            if group + 1 < groups - 1:
                over_cross(rest(group + 1))
            if group + 1 == groups - 1:
                over_cross_last(rest(group + 1))
            if group + 2 < groups:
                over_beside(rest(group + 2))

        row, size = bands[group]
        with jax.named_scope(f"fft#g={group}"):
            for a in range(side):
                cells_by_row[pl.ds(row * pitch + a, size, stride=pitch), :] = back[
                    row : row + size, a * side : (a + 1) * side
                ]
            filt_r = jnp.concatenate([filter_real[...]] * 2, axis=0)
            filt_i = jnp.concatenate([filter_imag[...]] * 2, axis=0)
            starts = range(row, row + size, 4)
            held = [
                jnp.concatenate(
                    [
                        jnp.concatenate(
                            [cells_by_row[cells_of(at)], cells_by_row[cells_of(at + 2)]], axis=1
                        ),
                        jnp.concatenate(
                            [cells_by_row[cells_of(at + 1)], cells_by_row[cells_of(at + 3)]], axis=1
                        ),
                    ],
                    axis=0,
                )
                for at in starts
            ]
            held = [first_turn(cells) for cells in held]
            held = [mm3(split_bf16(cells), loaded(inverse_table)) for cells in held]
            held = [
                (
                    spec[:, :side] * filt_r - spec[:, side:] * filt_i,
                    spec[:, :side] * filt_i + spec[:, side:] * filt_r,
                )
                for spec in held
            ]
            held = [back_turn(real, imag) for real, imag in held]
            held = [mm3(loaded(inverse_table), split_bf16(cells)) for cells in held]
            for at, done in zip(starts, held):
                cells_by_row[cells_of(at)] = done[:side, :side]
                cells_by_row[cells_of(at + 1)] = done[side:, :side]
                cells_by_row[cells_of(at + 2)] = done[:side, side:]
                cells_by_row[cells_of(at + 3)] = done[side:, side:]
            if (row + size) % 8 == 0:
                base = row + size - 8
                for a in range(side):
                    cut = slice(a * side, (a + 1) * side)
                    out[base : base + 8, cut] += cells_by_row[
                        pl.ds(base * pitch + a, 8, stride=pitch), :
                    ]

    with jax.named_scope("drain"):
        all_sent(send_back)


def fits(pixels, row_taps, column_taps):
    rows_dev, row_length = pixels.shape
    count = lax.axis_size("rows")
    side = math.isqrt(row_length)
    return (
        side == 128
        and side * side == row_length
        and row_length % (count * 1024) == 0
        and rows_dev % 16 == 0
        and 128 % rows_dev == 0
        and (count * rows_dev) % 128 == 0
        and count % (128 // rows_dev) == 0
        and count == 16
    )


def fused(pixels, row_taps, column_taps, stencil):
    rows_dev, row_length = pixels.shape
    count = lax.axis_size("rows")
    side = math.isqrt(row_length)
    column_length = rows_dev * count
    cols_dev = row_length // count
    a_dev = cols_dev // 128
    groups = len(bands_of(rows_dev))
    cuts = cuts_of(cols_dev)
    pieces = len(cuts)
    made = host_tables(side)
    tables = jnp.asarray(np.stack(made[:4]))
    twists = jnp.asarray(np.stack(made[4:]))
    hbm = pl.BlockSpec(memory_space=pltpu.HBM)
    vmem = pl.BlockSpec(memory_space=pltpu.VMEM)
    f32, bf16 = jnp.float32, jnp.bfloat16
    dma = pltpu.SemaphoreType.DMA
    return pl.pallas_call(
        functools.partial(kernel, (count, rows_dev, side)),
        out_shape=jax.ShapeDtypeStruct(pixels.shape, f32),
        in_specs=[hbm] * 6,
        out_specs=vmem,
        scratch_shapes=[
            pltpu.VMEM((rows_dev + 16, row_length), f32),
            pltpu.VMEM(tables.shape, bf16),
            pltpu.VMEM(twists.shape, f32),
            pltpu.VMEM((1, row_length), f32),
            pltpu.VMEM((1, row_length), f32),
            pltpu.VMEM((column_length, cols_dev), f32),
            pltpu.VMEM((column_length, cuts[0][1]), bf16),
            pltpu.VMEM((column_length, cuts[0][1]), bf16),
            pltpu.VMEM((column_length, cols_dev), f32),
            pltpu.VMEM((rows_dev, row_length), f32),
            pltpu.VMEM((rows_dev * (side + 8), side), f32),
            pltpu.VMEM((1, row_length), f32),
            pltpu.VMEM((1, row_length), f32),
            pltpu.VMEM((count, a_dev, 128), f32),
            pltpu.VMEM((count, 1, rows_dev), f32),
            pltpu.VMEM((column_length, column_length), bf16),
            pltpu.VMEM((column_length, column_length), bf16),
            pltpu.VMEM((side, side), f32),
            pltpu.VMEM((side, side), f32),
            pltpu.SMEM((3, 3), f32),
            dma,
            dma((pieces,)),
            dma,
            dma,
            dma((3,)),
            dma,
            dma((2,)),
            dma((2,)),
            dma,
            dma((groups,)),
            dma((7,)),
            pltpu.SemaphoreType.REGULAR((count // 2,)),
        ],
        compiler_params=pltpu.CompilerParams(
            collective_id=0, has_side_effects=True, vmem_limit_bytes=32 * 1024 * 1024
        ),
    )(
        *(
            pltpu.with_memory_space_constraint(operand, pltpu.HBM)
            for operand in (
                pixels,
                row_taps.reshape(a_dev, 128),
                column_taps.reshape(1, rows_dev),
                stencil,
                tables,
                twists,
            )
        )
    )


def chosen(pixels, row_taps, column_taps, stencil):
    if fits(pixels, row_taps, column_taps):
        return fused(pixels, row_taps, column_taps, stencil)
    return body(pixels, row_taps, column_taps, stencil)


def solution(mesh):
    in_specs = (
        P(("chan", "rows"), None),
        P(("chan", "rows")),
        P(("chan", "rows")),
        P("chan", None),
    )
    out_specs = P(("chan", "rows"), None)
    return jax.shard_map(chosen, mesh=mesh, in_specs=in_specs, out_specs=out_specs, check_vma=False)
```
